32 devices in a mesh: row: 4 (over y, x), col: 8 (over z, core).
Axes of the slice: x: 2, y: 2, z: 4, core: 2. Of those that a mesh axis runs over, the one named last changes fastest.
Arguments:
- tiles: bfloat16 [1024, 256, 256], P(('row', 'col')), as said below
- tile_row: int32 [1024], P(('row', 'col')), may hold values from 0 to 31, as said below
- tile_col: int32 [1024], P(('row', 'col')), may hold values from 0 to 31, as said below
- label_class: int32 [8192], P(('row', 'col')), may hold values from -1 to 127, as said below
Outputs:
- scores: float32 [8192, 128], P(('row', 'col'))
- residual: float32 [8192, 128], P(('row', 'col'))
The draws below stay inside these ranges and needn't reach their ends.
Inputs may be any that keep to these rules, and one draw needn't show every extreme that they name: `tiles`: Nonnegative. The tile of blocks (j, i) is the transpose of the tile of blocks (i, j); a tile on the diagonal is symmetric. No pair of blocks appears twice; the pair (j, i) is stored whenever (i, j) is. The device with row index r and col index c holds 32 tiles, all with tile_row // 8 == r and tile_col % 8 == c. `tile_col`: see tile_row. `label_class`: exactly 1024 nodes are labeled, and every class labels at least one node.
All inputs are finite; a program needn't handle non-finite values.
Results may differ from the reference program's by a relative error of at most 0.00062.
Values may be sent and summed in bfloat16 or wider, within the bound.
A program may use at most 64 MiB of HBM per device.

```python
import jax
import jax.numpy as jnp
from jax import lax

TILE = 256
CLASSES = 128
ITERS = 3
BLOCKS = 32
TILES_DEV = 32
NODES = 8192
N_COL = 8


def tile_pattern(key):
    pair_count = (TILES_DEV - 2) // 2
    shuffled = jax.random.permutation(jax.random.fold_in(key, 11), BLOCKS // 2 - 1) + 1
    chosen = shuffled[:pair_count].astype(jnp.int32)
    offsets = jnp.concatenate([jnp.array([0, BLOCKS // 2], jnp.int32), chosen, BLOCKS - chosen]).astype(jnp.int32)
    device = jnp.arange(BLOCKS, dtype=jnp.int32)[:, None]
    row_index = device // N_COL
    col_index = device % N_COL
    col_part = (col_index - offsets[None, :]) % N_COL
    rows = row_index * N_COL + col_part
    cols = (rows + offsets[None, :]) % BLOCKS
    return (rows.reshape(-1).astype(jnp.int32), cols.reshape(-1).astype(jnp.int32))


def draw_tile_row(key, part):
    return tile_pattern(key)[0]


def draw_tile_col(key, part):
    return tile_pattern(key)[1]


def draw_tiles(key, part):
    rows, cols = tile_pattern(key)
    smaller = jnp.minimum(rows, cols)
    larger = jnp.maximum(rows, cols)
    pair_id = smaller * BLOCKS + larger
    scale_value = 400.0 * CLASSES / (TILES_DEV * TILE)

    def one_tile(element):
        pair_value, transposed, on_diagonal = element
        pair_key = jax.random.fold_in(jax.random.fold_in(key, 23), pair_value)
        first_key, second_key = jax.random.split(pair_key)
        entries = jnp.exp(-6.0 * jax.random.uniform(first_key, (TILE, TILE), jnp.float32))
        factor = jnp.exp(jnp.log(0.01) * jax.random.uniform(second_key, (), jnp.float32))
        entries = entries * factor
        entries = jnp.where(on_diagonal, 0.5 * (entries + entries.T), jnp.where(transposed, entries.T, entries))
        return (entries * scale_value).astype(jnp.bfloat16)
    return lax.map(one_tile, (pair_id, rows > cols, rows == cols))


def draw_label_class(key, part):
    shuffled = jax.random.permutation(jax.random.fold_in(key, 5), NODES)
    random_class = jax.random.randint(jax.random.fold_in(key, 6), (NODES,), 0, CLASSES)
    ranking = jnp.arange(NODES, dtype=jnp.int32)
    assigned = jnp.where(ranking < CLASSES, ranking, random_class)
    assigned = jnp.where(ranking < NODES // 8, assigned, -1).astype(jnp.int32)
    return jnp.zeros((NODES,), jnp.int32).at[shuffled].set(assigned)


def setup_inputs(seed: int = 0) -> dict:
    splits = jax.random.split(jax.random.key(seed), 5)
    tiles = draw_tiles(jax.random.fold_in(splits[4], 71), 0)
    tile_row = draw_tile_row(jax.random.fold_in(splits[4], 71), 0)
    tile_col = draw_tile_col(jax.random.fold_in(splits[4], 71), 0)
    label_class = draw_label_class(jax.random.fold_in(splits[4], 71), 0)
    return {"tiles": tiles, "tile_row": tile_row, "tile_col": tile_col, "label_class": label_class}


def weight_apply(tiles, tile_row, tile_col, vector_half):
    source = vector_half.reshape(BLOCKS, TILE, CLASSES).astype(jnp.float32)
    grouped = tiles.reshape(BLOCKS, TILES_DEV, TILE, TILE)
    grouped_rows = tile_row.reshape(BLOCKS, TILES_DEV).astype(jnp.int32)
    grouped_cols = tile_col.reshape(BLOCKS, TILES_DEV).astype(jnp.int32)

    def one_group(running, element):
        tile_block, block_row, block_col = element
        products = jnp.einsum("tab,tbk->tak", tile_block.astype(jnp.float32), source[block_col], precision=lax.Precision.HIGHEST)
        return running.at[block_row].add(products), None

    start = jnp.zeros((BLOCKS, TILE, CLASSES), jnp.float32)
    running, _ = lax.scan(one_group, start, (grouped, grouped_rows, grouped_cols))
    return running.reshape(NODES, CLASSES)


def reference(tiles, tile_row, tile_col, label_class):
    row_sums = jnp.sum(tiles.astype(jnp.float32), axis=2)
    degree = jax.ops.segment_sum(row_sums, tile_row.astype(jnp.int32), num_segments=BLOCKS).reshape(NODES)
    unlabeled = label_class < 0
    onehot = (label_class[:, None] == jnp.arange(CLASSES, dtype=jnp.int32)[None, :]).astype(jnp.bfloat16)
    rhs = jnp.where(unlabeled[:, None], weight_apply(tiles, tile_row, tile_col, onehot), jnp.float32(0.0))

    def operator(direction):
        mixed = weight_apply(tiles, tile_row, tile_col, direction.astype(jnp.bfloat16))
        return jnp.where(unlabeled[:, None], degree[:, None] * direction - mixed, direction)

    solution = jnp.zeros((NODES, CLASSES), jnp.float32)
    residual = rhs
    direction = rhs
    norm_now = jnp.sum(residual * residual, axis=0)
    for iteration in range(ITERS):
        image = operator(direction)
        alpha = norm_now / jnp.sum(direction * image, axis=0)
        solution = solution + alpha * direction
        residual = residual - alpha * image
        norm_next = jnp.sum(residual * residual, axis=0)
        direction = residual + (norm_next / norm_now) * direction
        norm_now = norm_next
    return 8.0 * CLASSES * solution, residual
```

```python
import functools

import jax
import jax.numpy as jnp
from jax import lax
from jax.experimental import pallas as pl
from jax.experimental.pallas import tpu as pltpu
from jax.sharding import PartitionSpec as P

CLASSES = 128
ITERS = 3
PAD = 16
DEG = 8
UNROLL = 32
PARTS = 4
CHAINS = 4
LIMIT = 32700.0
OFFSET = 1.4
NEAR, FAR, READY, PERIOD = 2.8, 5.0, 6.5, 10.2


def flip(index, mask):
    bit = 1
    result = index
    while bit <= mask:
        if mask & bit:
            result = result + bit * (1 - 2 * lax.rem(lax.div(index, bit), 2))
        bit *= 2
    return result


def kernel(
    R, C, pos, label_ref, tiles_hbm, x_out, r_out,
    tiles, lab, hot, acc0, rs0, code, unit, panel, rep_r, rep_p, acc, rs, st_a, st_c,
    degree, direction, image, residual, answer,
    tile_sem, lab_send, lab_recv, code_send, code_recv, unit_send, unit_recv, deg_send, rs0_send, rs0_recv, rs_send, rs_recv,
    sta_send, sta_recv, stc_send, stc_recv,
):
    T, B = tiles_hbm.shape[0], tiles_hbm.shape[1]
    Z = C // 2
    K, H = CLASSES, CLASSES // CHAINS
    Q = K // H
    G = H // 2
    f32, bf16, i32 = jnp.float32, jnp.bfloat16, jnp.int32
    unroll = R * C <= UNROLL
    row, col = lax.axis_index("row"), lax.axis_index("col")
    core = lax.rem(col, 2)
    chip = lax.div(col, 2)
    peer = col + 1 - 2 * core
    assert C % 2 == 0 and C & (C - 1) == 0 and R & (R - 1) == 0

    def col_partner(m):
        return flip(col, m)

    def row_partner(m):
        return flip(row, m)

    def loop(count, body, carry):
        if unroll:
            for n in range(count):
                carry = body(n, carry)
            return carry
        return lax.fori_loop(0, count, body, carry)

    step = -(-T // PARTS)
    for p in range(PARTS):
        lo, hi = p * step, min(T, (p + 1) * step)
        if lo < hi:
            pltpu.make_async_copy(
                tiles_hbm.at[pl.ds(lo, hi - lo)], tiles.at[pl.ds(lo, hi - lo)], tile_sem.at[0]
            ).start()
    if tiles.shape[0] > T:
        tiles[T] = jnp.zeros((B, B), bf16)

    barrier = pltpu.get_barrier_semaphore()
    for m in range(1, C):
        pl.semaphore_signal(
            barrier, inc=1, device_id={"col": col_partner(m)}, device_id_type=pl.DeviceIdType.MESH
        )
    for m in range(1, R):
        pl.semaphore_signal(
            barrier, inc=1, device_id={"row": row_partner(m)}, device_id_type=pl.DeviceIdType.MESH
        )
    mine = label_ref[...]
    lab[col] = jnp.broadcast_to(mine, (8, B))
    pl.semaphore_wait(barrier, C - 1 + R - 1)

    def send(src, dst, send_sem, recv_sem, where):
        pltpu.make_async_remote_copy(
            src_ref=src, dst_ref=dst, send_sem=send_sem, recv_sem=recv_sem,
            device_id=where, device_id_type=pl.DeviceIdType.MESH,
        ).start()

    def landed(ref, recv_sem):
        pltpu.make_async_remote_copy(
            src_ref=ref, dst_ref=ref, send_sem=tile_sem.at[0], recv_sem=recv_sem,
            device_id={"col": peer}, device_id_type=pl.DeviceIdType.MESH,
        ).wait_recv()

    def drained(ref, send_sem):
        pltpu.make_async_remote_copy(
            src_ref=ref, dst_ref=ref, send_sem=send_sem, recv_sem=tile_sem.at[0],
            device_id={"col": peer}, device_id_type=pl.DeviceIdType.MESH,
        ).wait_send()

    def other_chip(j):
        upper = lax.div(2 * chip, Z)
        low = chip + upper * (Z - 1 - 2 * chip)
        far = Z - 1 - j - lax.div(low + j + 1, Z)
        return far + upper * (Z - 1 - 2 * far)

    def tile_at(source, k):
        return tiles[pos[source * R + k]]

    def fold(product):
        folded = product[:, :K]
        for lane in range(K, B, K):
            folded = folded + product[:, lane : lane + K]
        return folded

    def sums_row(products):
        rows = []
        for lo in range(0, len(products), Q):
            part = [fold(p) for p in products[lo : lo + Q]]
            if len(part) < Q:
                part.append(jnp.zeros((K - H * len(part), K), f32))
            rows.append(jnp.sum(jnp.concatenate(part, axis=0).T, axis=0, keepdims=True))
        return rows

    def spread(rows, count):
        values = []
        for q in range(count):
            if q % Q == 0:
                square = jnp.broadcast_to(rows[q // Q], (K, K)).T
            values.append(square[q % Q * H : (q % Q + 1) * H])
        return values

    def wide(value):
        return jnp.concatenate([value] * (B // K), axis=1)

    def encode(t, value):
        top = jnp.clip(jnp.max(jnp.abs(value), axis=0, keepdims=True), 2.0**-100, 2.0**120)
        power = jnp.ceil(jnp.log2(top))
        whole = jnp.round(value * (jnp.exp2(-power) * LIMIT)).astype(i32)
        code[t, col] = (whole[:G] << 16) | (whole[G:] & 0xFFFF)
        unit[t, col] = jnp.exp2(power) * (1.0 / LIMIT)

    def decode(t, c):
        word = code[t, c]
        scale = unit[t, c]
        high = (word >> 16).astype(f32) * scale
        low = ((word << 16) >> 16).astype(f32) * scale
        return jnp.concatenate([high, low], axis=0)

    for m in range(C - 1, 0, -1):
        send(lab.at[col], lab.at[col], lab_send.at[0], lab_recv.at[col], {"col": col_partner(m)})
    class_axis = lax.broadcasted_iota(i32, (K, B), 0)
    ones = jnp.ones((PAD, B), bf16)

    def show(c):
        value = jnp.where(lab[c][0:1] == class_axis, 1.0, 0.0).astype(bf16)
        hot[c] = jnp.concatenate([ones, value], axis=0)

    show(col)
    free = jnp.broadcast_to(mine, (H, B)) < 0
    pltpu.make_async_copy(tiles, tiles, tile_sem.at[0]).wait() if tiles.shape[0] == T else pltpu.make_async_copy(
        tiles.at[pl.ds(0, T)], tiles.at[pl.ds(0, T)], tile_sem.at[0]
    ).wait()

    bounds = [0, min(2, C), min(6, C), C]
    for lo, hi in zip(bounds, bounds[1:]):
        for m in range(max(lo, 1), hi):
            c = col_partner(m)
            landed(lab.at[c], lab_recv.at[c])
            show(c)
        if hi > lo:
            for m in range(R - 1, -1, -1):
                k = row_partner(m)
                value = None if lo == 0 else acc0[k]
                for n in range(lo, hi):
                    c = col_partner(n) if n else col
                    part = jnp.dot(hot[c], tile_at(c, k), preferred_element_type=f32)
                    value = part if value is None else value + part
                acc0[k] = value

    def first_rows(h):
        return (PAD - DEG, H + DEG) if h == 0 else (PAD + h * H, H)

    for h in range(CHAINS):
        lo, size = first_rows(h)
        for m in range(R - 1, 0, -1):
            k = row_partner(m)
            send(
                acc0.at[k, pl.ds(lo, size)], rs0.at[h, m - 1, pl.ds(0, size)],
                deg_send.at[0] if h == 0 else rs0_send.at[0], rs0_recv.at[h], {"row": k},
            )

    def gather_start(t):
        own = code.at[t, col]
        for j in range(Z - 1):
            send(own, own, code_send.at[0], code_recv.at[t, chip], {"col": 2 * other_chip(j) + core})
        send(own, own, code_send.at[0], code_recv.at[t, chip], {"col": peer})
        own = unit.at[t, col]
        for m in range(C - 1, 0, -1):
            send(own, own, unit_send.at[0], unit_recv.at[t], {"col": col_partner(m)})

    def gather_relay(t, j):
        z = other_chip(j)
        block = code.at[t, 2 * z + core]
        landed(block, code_recv.at[t, z])
        send(block, block, code_send.at[0], code_recv.at[t, chip], {"col": peer})

    def gather_end(t):
        landed(code.at[t, pl.ds(0, Z)], code_recv.at[t, chip])
        landed(unit.at[t, pl.ds(0, C - 1)], unit_recv.at[t])

    def stats_start(t, rows):
        for i in range(st_a.shape[2]):
            st_a[t, row, i] = rows[i] if i < len(rows) else jnp.zeros((1, K), f32)
        own = st_a.at[t, row]
        for m in range(R - 1, 0, -1):
            send(own, own, sta_send.at[0], sta_recv.at[t], {"row": row_partner(m)})

    def stats_middle(t):
        landed(st_a.at[t, pl.ds(0, R - 1)], sta_recv.at[t])
        st_c[t, col] = jnp.sum(st_a[t], axis=0)
        own = st_c.at[t, col]
        for m in range(C - 1, 0, -1):
            send(own, own, stc_send.at[0], stc_recv.at[t], {"col": col_partner(m)})

    def stats_end(t):
        landed(st_c.at[t, pl.ds(0, C - 1)], stc_recv.at[t])
        return jnp.sum(st_c[t], axis=0)

    def chain(h):
        clock = h * OFFSET
        yield clock
        lo, size = first_rows(h)
        landed(rs0.at[h, :, pl.ds(0, size)], rs0_recv.at[h])
        value = acc0[row, lo : lo + size]
        for m in range(1, R):
            value = value + rs0[h, m - 1, 0:size]
        if h == 0:
            degree[...] = value[:DEG]
            value = value[DEG:]
        rhs = jnp.where(free, value, 0.0)
        encode(h * ITERS, rhs)
        gather_start(h * ITERS)
        answer[h] = jnp.zeros((H, B), f32)
        residual[h] = rhs
        direction[h] = rhs
        norm = alpha = beta = None
        for s in range(ITERS):
            t = h * ITERS + s
            last = s + 1 == ITERS
            yield clock + NEAR
            for j in range(Z - 2, 0, -1):
                gather_relay(t, j)
            if s:
                stats_middle(t - 1)
            yield clock + FAR
            if Z > 1:
                gather_relay(t, 0)
            yield clock + READY
            if s:
                total = stats_end(t - 1)
                if s == 1:
                    di, ii, norm = spread(total, 3)
                    ri = di
                else:
                    di, ri, ii = spread(total, 3)
                alpha = norm / di
                after = norm - 2.0 * alpha * ri + alpha * alpha * ii
                beta = after / norm
                norm = after
                a, b = wide(alpha), wide(beta)
            gather_end(t)

            def refresh(c, carry):
                fresh = decode(t, c)
                if s == 0:
                    rep_r[h, c] = fresh
                else:
                    old = rep_r[h, c]
                    r = old - a * fresh
                    p = r + b * (old if s == 1 else rep_p[h, c])
                    if not last:
                        rep_r[h, c] = r
                        rep_p[h, c] = p
                    fresh = p
                panel[h, c] = fresh.astype(bf16)
                return carry

            loop(C, refresh, 0)
            for m in range(R - 1, -1, -1):
                k = row_partner(m)

                def one(c, value):
                    part = jnp.dot(panel[h, c], tile_at(c, k), preferred_element_type=f32)
                    return part if value is None else value + part

                acc[t, k] = loop(C, one, None if unroll else jnp.zeros((H, B), f32))
                if m:
                    send(acc.at[t, k], rs.at[t, m - 1], rs_send.at[0], rs_recv.at[t], {"row": k})
            if s:
                d = direction[h]
                r = residual[h] - a * image[h]
                answer[h] = answer[h] + a * d
                residual[h] = r
                direction[h] = r + b * d
            clock += PERIOD
            yield clock
            landed(rs.at[t], rs_recv.at[t])
            mixed = acc[t, row]
            for m in range(1, R):
                mixed = mixed + rs[t, m - 1]
            d = direction[h]
            i = jnp.where(free, degree[0:1] * d - mixed, d)
            if not last:
                encode(t + 1, i)
                gather_start(t + 1)
            image[h] = i
            if last:
                products = [d * i]
            else:
                r = residual[h]
                products = [d * i, i * i, r * r] if s == 0 else [d * i, r * i, i * i]
            stats_start(t, sums_row(products))
        yield clock + NEAR
        stats_middle(t)
        yield clock + READY
        (di,) = spread(stats_end(t), 1)
        a = wide(norm / di)
        x_out[:, h * H : (h + 1) * H] = ((8.0 * K) * (answer[h] + a * direction[h])).T
        r_out[:, h * H : (h + 1) * H] = (residual[h] - a * image[h]).T

    queue = []
    for h in range(CHAINS):
        one = chain(h)
        queue.append((next(one), h, one))
    while queue:
        queue.sort(key=lambda entry: entry[:2])
        _, h, one = queue.pop(0)
        when = next(one, None)
        if when is not None:
            queue.append((when, h, one))

    drained(lab.at[pl.ds(0, C - 1)], lab_send.at[0])
    drained(code.at[:, pl.ds(0, C - 1)], code_send.at[0])
    drained(unit.at[:, pl.ds(0, C - 1)], unit_send.at[0])
    drained(rs0.at[0], deg_send.at[0])
    if CHAINS > 1:
        drained(rs0.at[pl.ds(0, CHAINS - 1), :, pl.ds(0, H)], rs0_send.at[0])
    drained(rs, rs_send.at[0])
    drained(st_a.at[:, pl.ds(0, R - 1)], sta_send.at[0])
    drained(st_c.at[:, pl.ds(0, C - 1)], stc_send.at[0])


def solution(mesh):
    R, C = mesh.shape["row"], mesh.shape["col"]

    def shards(tiles, tile_row, tile_col, label_class):
        T, B = tiles.shape[0], tiles.shape[1]
        K, H, N = CLASSES, CLASSES // CHAINS, CHAINS
        place = lax.rem(tile_row, C) * R + lax.div(tile_col, C)
        slot = lax.broadcasted_iota(jnp.int32, (R * C, T), 0)
        index = lax.broadcasted_iota(jnp.int32, (R * C, T), 1)
        held = T if T == R * C else T + 1
        miss = held - 1 if held > T else 0
        pos = jnp.sum(jnp.where(place[None, :] == slot, index - miss, 0), axis=1)
        if miss:
            pos = pos + miss
        f32, bf16, i32 = jnp.float32, jnp.bfloat16, jnp.int32
        dma = pltpu.SemaphoreType.DMA
        vmem = pl.BlockSpec(memory_space=pltpu.VMEM)
        node = pltpu.VMEM((N, H, B), f32)
        steps = N * ITERS
        lines = -(-3 // (K // H))
        return pl.pallas_call(
            functools.partial(kernel, R, C),
            out_shape=(jax.ShapeDtypeStruct((B, K), f32), jax.ShapeDtypeStruct((B, K), f32)),
            in_specs=[
                pl.BlockSpec(memory_space=pltpu.SMEM),
                vmem,
                pl.BlockSpec(memory_space=pl.ANY),
            ],
            out_specs=(vmem, vmem),
            scratch_shapes=[
                pltpu.VMEM((held, B, B), bf16),
                pltpu.VMEM((C, 8, B), i32),
                pltpu.VMEM((C, PAD + K, B), bf16),
                pltpu.VMEM((R, PAD + K, B), f32),
                pltpu.VMEM((N, R - 1, H + DEG, B), f32),
                pltpu.VMEM((steps, C, H // 2, B), i32),
                pltpu.VMEM((steps, C, 1, B), f32),
                pltpu.VMEM((N, C, H, B), bf16),
                pltpu.VMEM((N, C, H, B), f32),
                pltpu.VMEM((N, C, H, B), f32),
                pltpu.VMEM((steps, R, H, B), f32),
                pltpu.VMEM((steps, R - 1, H, B), f32),
                pltpu.VMEM((steps, R, lines, 1, K), f32),
                pltpu.VMEM((steps, C, lines, 1, K), f32),
                pltpu.VMEM((DEG, B), f32),
                node, node, node, node,
                dma((1,)),
                dma((1,)), dma((C,)),
                dma((1,)), dma((steps, C // 2)),
                dma((1,)), dma((steps,)),
                dma((1,)), dma((1,)), dma((N,)),
                dma((1,)), dma((steps,)),
                dma((1,)), dma((steps,)),
                dma((1,)), dma((steps,)),
            ],
            compiler_params=pltpu.CompilerParams(
                collective_id=0, has_side_effects=True, vmem_limit_bytes=63 * 1024 * 1024
            ),
        )(pos.astype(jnp.int32), label_class.reshape(1, B), tiles)

    placed = (P(("row", "col"), None, None),) + (P(("row", "col")),) * 3
    return jax.shard_map(
        shards,
        mesh=mesh,
        in_specs=placed,
        out_specs=(P(("row", "col"), None), P(("row", "col"), None)),
        check_vma=False,
    )
```

```python
import functools

import jax
import jax.numpy as jnp
from jax import lax
from jax.experimental import pallas as pl
from jax.experimental.pallas import tpu as pltpu
from jax.sharding import PartitionSpec as P

CLASSES = 128
ITERS = 3
PAD = 16
DEG = 8
UNROLL = 32
PARTS = 4
CHAINS = 4
LIMIT = 32700.0
OFFSET = 2.5
NEAR, MID, FAR, READY, PERIOD, SUMS = 2.8, 2.8, 5.0, 6.5, 10.2, 5.8


def flip(index, mask):
    bit = 1
    result = index
    while bit <= mask:
        if mask & bit:
            result = result + bit * (1 - 2 * lax.rem(lax.div(index, bit), 2))
        bit *= 2
    return result


def kernel(
    R, C, row_hbm, col_hbm, label_hbm, tiles_hbm, x_out, r_out,
    tile_row, tile_col, pos, label_ref,
    tiles, lab, hot, acc0, rs0, code, unit, panel, rep_r, rep_p, acc, rs, st,
    degree, direction, image, residual, answer,
    tile_sem, lab_send, lab_recv, code_send, code_recv, unit_send, unit_recv, deg_send, rs0_send, rs0_recv, rs_send, rs_recv,
    st_send, st_recv, in_sem,
):
    T, B = tiles_hbm.shape[0], tiles_hbm.shape[1]
    Z = C // 2
    K, H = CLASSES, CLASSES // CHAINS
    Q = K // H
    G = H // 2
    f32, bf16, i32 = jnp.float32, jnp.bfloat16, jnp.int32
    unroll = R * C <= UNROLL
    row, col = lax.axis_index("row"), lax.axis_index("col")
    core = lax.rem(col, 2)
    chip = lax.div(col, 2)
    peer = col + 1 - 2 * core
    assert C % 2 == 0 and C & (C - 1) == 0 and R & (R - 1) == 0

    def col_partner(m):
        return flip(col, m)

    def row_partner(m):
        return flip(row, m)

    def loop(count, body, carry):
        if unroll:
            for n in range(count):
                carry = body(n, carry)
            return carry
        return lax.fori_loop(0, count, body, carry)

    inputs = [
        pltpu.make_async_copy(source, target, in_sem.at[n])
        for n, (source, target) in enumerate(
            [(label_hbm, label_ref), (row_hbm, tile_row), (col_hbm, tile_col)]
        )
    ]
    for cp in inputs:
        cp.start()
    barrier = pltpu.get_barrier_semaphore()
    for m in range(C - 1, 0, -1):
        pl.semaphore_signal(
            barrier, inc=1, device_id={"col": col_partner(m)}, device_id_type=pl.DeviceIdType.MESH
        )
    for m in range(R - 1, 0, -1):
        pl.semaphore_signal(
            barrier, inc=1, device_id={"row": row_partner(m)}, device_id_type=pl.DeviceIdType.MESH
        )
    step = -(-T // PARTS)
    for p in range(PARTS):
        lo, hi = p * step, min(T, (p + 1) * step)
        if lo < hi:
            pltpu.make_async_copy(
                tiles_hbm.at[pl.ds(lo, hi - lo)], tiles.at[pl.ds(lo, hi - lo)], tile_sem.at[0]
            ).start()
    if tiles.shape[0] > T:
        tiles[T] = jnp.zeros((B, B), bf16)
    for cp in inputs:
        cp.wait()
    mine = label_ref[...]
    lab[col] = mine

    def place(n, carry):
        tile_row[n] = lax.rem(tile_row[n], C) * R + lax.div(tile_col[n], C)
        return carry

    lax.fori_loop(0, T, place, 0)
    miss = tiles.shape[0] - 1

    def locate(slot, carry):
        found = miss
        for n in range(T):
            found = jnp.minimum(found, jnp.where(tile_row[n] == slot, n, miss))
        pos[slot] = found
        return carry

    lax.fori_loop(0, R * C, locate, 0)
    pl.semaphore_wait(barrier, C - 1 + R - 1)

    def send(src, dst, send_sem, recv_sem, where):
        pltpu.make_async_remote_copy(
            src_ref=src, dst_ref=dst, send_sem=send_sem, recv_sem=recv_sem,
            device_id=where, device_id_type=pl.DeviceIdType.MESH,
        ).start()

    def landed(ref, recv_sem):
        pltpu.make_async_remote_copy(
            src_ref=ref, dst_ref=ref, send_sem=tile_sem.at[0], recv_sem=recv_sem,
            device_id={"col": peer}, device_id_type=pl.DeviceIdType.MESH,
        ).wait_recv()

    def drained(ref, send_sem):
        pltpu.make_async_remote_copy(
            src_ref=ref, dst_ref=ref, send_sem=send_sem, recv_sem=tile_sem.at[0],
            device_id={"col": peer}, device_id_type=pl.DeviceIdType.MESH,
        ).wait_send()

    def other_chip(j):
        upper = lax.div(2 * chip, Z)
        low = chip + upper * (Z - 1 - 2 * chip)
        far = Z - 1 - j - lax.div(low + j + 1, Z)
        return far + upper * (Z - 1 - 2 * far)

    def tile_at(source, k):
        return tiles[pos[source * R + k]]

    def fold(product):
        folded = product[:, :K]
        for lane in range(K, B, K):
            folded = folded + product[:, lane : lane + K]
        return folded

    def sums_row(products):
        rows = []
        for lo in range(0, len(products), Q):
            part = [fold(p) for p in products[lo : lo + Q]]
            if len(part) < Q:
                part.append(jnp.zeros((K - H * len(part), K), f32))
            rows.append(jnp.sum(jnp.concatenate(part, axis=0).T, axis=0, keepdims=True))
        return rows

    def spread(rows, count):
        values = []
        for q in range(count):
            if q % Q == 0:
                square = jnp.broadcast_to(rows[q // Q], (K, K)).T
            values.append(square[q % Q * H : (q % Q + 1) * H])
        return values

    def wide(value):
        return jnp.concatenate([value] * (B // K), axis=1)

    def encode(t, value):
        top = jnp.clip(jnp.max(jnp.abs(value), axis=0, keepdims=True), 2.0**-100, 2.0**120)
        power = jnp.ceil(jnp.log2(top))
        whole = jnp.round(value * (jnp.exp2(-power) * LIMIT)).astype(i32)
        code[t, col] = (whole[:G] << 16) | (whole[G:] & 0xFFFF)
        unit[t, col] = jnp.exp2(power) * (1.0 / LIMIT)

    def decode(t, c):
        word = code[t, c]
        scale = unit[t, c]
        high = (word >> 16).astype(f32) * scale
        low = ((word << 16) >> 16).astype(f32) * scale
        return jnp.concatenate([high, low], axis=0)

    for m in range(C - 1, 0, -1):
        send(lab.at[col], lab.at[col], lab_send.at[0], lab_recv.at[col], {"col": col_partner(m)})
    class_axis = lax.broadcasted_iota(i32, (K, B), 0)
    ones = jnp.ones((PAD, B), bf16)

    def show(c):
        value = jnp.where(lab[c] == class_axis, 1.0, 0.0).astype(bf16)
        hot[c] = jnp.concatenate([ones, value], axis=0)

    show(col)
    free = jnp.broadcast_to(mine, (H, B)) < 0
    pltpu.make_async_copy(tiles, tiles, tile_sem.at[0]).wait() if tiles.shape[0] == T else pltpu.make_async_copy(
        tiles.at[pl.ds(0, T)], tiles.at[pl.ds(0, T)], tile_sem.at[0]
    ).wait()

    bounds = [0, min(2, C), min(6, C), C]
    for lo, hi in zip(bounds, bounds[1:]):
        for m in range(max(lo, 1), hi):
            c = col_partner(m)
            landed(lab.at[c], lab_recv.at[c])
            show(c)
        if hi > lo:
            for m in range(R - 1, -1, -1):
                k = row_partner(m)
                value = None if lo == 0 else acc0[k]
                for n in range(lo, hi):
                    c = col_partner(n) if n else col
                    part = jnp.dot(hot[c], tile_at(c, k), preferred_element_type=f32)
                    value = part if value is None else value + part
                acc0[k] = value

    def first_rows(h):
        return (PAD - DEG, H + DEG) if h == 0 else (PAD + h * H, H)

    for h in range(CHAINS):
        lo, size = first_rows(h)
        for m in range(R - 1, 0, -1):
            k = row_partner(m)
            send(
                acc0.at[k, pl.ds(lo, size)], rs0.at[h, m - 1, pl.ds(0, size)],
                deg_send.at[0] if h == 0 else rs0_send.at[0], rs0_recv.at[h], {"row": k},
            )

    def gather_start(t):
        own = code.at[t, col]
        for j in range(Z - 1):
            send(own, own, code_send.at[0], code_recv.at[t, chip], {"col": 2 * other_chip(j) + core})
        send(own, own, code_send.at[0], code_recv.at[t, chip], {"col": peer})
        own = unit.at[t, col]
        for m in range(C - 1, 0, -1):
            send(own, own, unit_send.at[0], unit_recv.at[t], {"col": col_partner(m)})

    def gather_relay(t, j):
        z = other_chip(j)
        block = code.at[t, 2 * z + core]
        landed(block, code_recv.at[t, z])
        send(block, block, code_send.at[0], code_recv.at[t, chip], {"col": peer})

    def gather_end(t):
        landed(code.at[t, pl.ds(0, Z)], code_recv.at[t, chip])
        landed(unit.at[t, pl.ds(0, C - 1)], unit_recv.at[t])

    me = row * C + col

    def stats_start(t, rows):
        for i in range(st.shape[2]):
            st[t, me, i] = rows[i] if i < len(rows) else jnp.zeros((1, K), f32)
        own = st.at[t, me]

        def out(n, carry):
            other = lax.rem(me + n + 1, R * C)
            send(own, own, st_send.at[0], st_recv.at[t], {"row": lax.div(other, C), "col": lax.rem(other, C)})
            return carry

        loop(R * C - 1, out, 0)

    def stats_end(t):
        landed(st.at[t, pl.ds(0, R * C - 1)], st_recv.at[t])
        return jnp.sum(st[t], axis=0)

    def chain(h):
        clock = OFFSET * h
        yield clock
        lo, size = first_rows(h)
        landed(rs0.at[h, :, pl.ds(0, size)], rs0_recv.at[h])
        value = acc0[row, lo : lo + size]
        for m in range(1, R):
            value = value + rs0[h, m - 1, 0:size]
        if h == 0:
            degree[...] = value[:DEG]
            value = value[DEG:]
        rhs = jnp.where(free, value, 0.0)
        encode(h * ITERS, rhs)
        gather_start(h * ITERS)
        answer[h] = jnp.zeros((H, B), f32)
        residual[h] = rhs
        direction[h] = rhs
        norm = None
        for s in range(ITERS):
            t = h * ITERS + s
            last = s + 1 == ITERS
            if Z > 1:
                yield clock + NEAR
                gather_relay(t, Z - 2)
            if Z > 2:
                yield clock + MID
                for j in range(Z - 3, 0, -1):
                    gather_relay(t, j)
                yield clock + FAR
                gather_relay(t, 0)
            yield clock + READY
            if s:
                total = stats_end(t - 1)
                if s == 1:
                    di, ii, norm = spread(total, 3)
                    ri = di
                else:
                    di, ri, ii = spread(total, 3)
                alpha = norm / di
                after = norm - 2.0 * alpha * ri + alpha * alpha * ii
                beta = after / norm
                norm = after
                a, b = wide(alpha), wide(beta)
            gather_end(t)

            def refresh(c, carry):
                fresh = decode(t, c)
                if s == 0:
                    rep_r[h, c] = fresh
                else:
                    old = rep_r[h, c]
                    r = old - a * fresh
                    p = r + b * (old if s == 1 else rep_p[h, c])
                    if not last:
                        rep_r[h, c] = r
                        rep_p[h, c] = p
                    fresh = p
                panel[h, c] = fresh.astype(bf16)
                return carry

            loop(C, refresh, 0)

            def ship(m, k, value):
                acc[t, k] = value
                if m:
                    send(acc.at[t, k], rs.at[t, m - 1], rs_send.at[0], rs_recv.at[t], {"row": k})

            held = None
            for m in range(R - 1, -1, -1):
                k = row_partner(m)

                def one(c, value):
                    part = jnp.dot(panel[h, c], tile_at(c, k), preferred_element_type=f32)
                    return part if value is None else value + part

                value = loop(C, one, None if unroll else jnp.zeros((H, B), f32))
                if held is not None:
                    ship(*held)
                held = (m, k, value)
            ship(*held)
            if s:
                d = direction[h]
                r = residual[h] - a * image[h]
                answer[h] = answer[h] + a * d
                residual[h] = r
                direction[h] = r + b * d
            clock += PERIOD
            yield clock
            landed(rs.at[t], rs_recv.at[t])
            mixed = acc[t, row]
            for m in range(1, R):
                mixed = mixed + rs[t, m - 1]
            d = direction[h]
            i = jnp.where(free, degree[0:1] * d - mixed, d)
            if not last:
                encode(t + 1, i)
                gather_start(t + 1)
            image[h] = i
            if last:
                products = [d * i]
            else:
                r = residual[h]
                products = [d * i, i * i, r * r] if s == 0 else [d * i, r * i, i * i]
            stats_start(t, sums_row(products))
        yield clock + SUMS
        (di,) = spread(stats_end(t), 1)
        a = wide(norm / di)
        x_out[:, h * H : (h + 1) * H] = ((8.0 * K) * (answer[h] + a * direction[h])).T
        r_out[:, h * H : (h + 1) * H] = (residual[h] - a * image[h]).T

    queue = []
    for h in range(CHAINS):
        one = chain(h)
        queue.append((next(one), h, one))
    while queue:
        queue.sort(key=lambda entry: entry[:2])
        _, h, one = queue.pop(0)
        when = next(one, None)
        if when is not None:
            queue.append((when, h, one))

    drained(lab.at[pl.ds(0, C - 1)], lab_send.at[0])
    drained(code.at[:, pl.ds(0, C - 1)], code_send.at[0])
    drained(unit.at[:, pl.ds(0, C - 1)], unit_send.at[0])
    drained(rs0.at[0], deg_send.at[0])
    if CHAINS > 1:
        drained(rs0.at[pl.ds(0, CHAINS - 1), :, pl.ds(0, H)], rs0_send.at[0])
    drained(rs, rs_send.at[0])
    drained(st.at[:, pl.ds(0, R * C - 1)], st_send.at[0])


def solution(mesh):
    R, C = mesh.shape["row"], mesh.shape["col"]

    def shards(tiles, tile_row, tile_col, label_class):
        T, B = tiles.shape[0], tiles.shape[1]
        K, H, N = CLASSES, CLASSES // CHAINS, CHAINS
        held = T if T == R * C else T + 1
        f32, bf16, i32 = jnp.float32, jnp.bfloat16, jnp.int32
        dma = pltpu.SemaphoreType.DMA
        vmem, hbm = pl.BlockSpec(memory_space=pltpu.VMEM), pl.BlockSpec(memory_space=pltpu.HBM)
        smem = pltpu.SMEM
        node = pltpu.VMEM((N, H, B), f32)
        steps = N * ITERS
        lines = -(-3 // (K // H))
        return pl.pallas_call(
            functools.partial(kernel, R, C),
            out_shape=(jax.ShapeDtypeStruct((B, K), f32), jax.ShapeDtypeStruct((B, K), f32)),
            in_specs=[
                hbm, hbm, hbm, hbm,
            ],
            out_specs=(vmem, vmem),
            scratch_shapes=[
                smem((T,), i32), smem((T,), i32), smem((R * C,), i32), pltpu.VMEM((1, B), i32),
                pltpu.VMEM((held, B, B), bf16),
                pltpu.VMEM((C, 1, B), i32),
                pltpu.VMEM((C, PAD + K, B), bf16),
                pltpu.VMEM((R, PAD + K, B), f32),
                pltpu.VMEM((N, R - 1, H + DEG, B), f32),
                pltpu.VMEM((steps, C, H // 2, B), i32),
                pltpu.VMEM((steps, C, 1, B), f32),
                pltpu.VMEM((N, C, H, B), bf16),
                pltpu.VMEM((N, C, H, B), f32),
                pltpu.VMEM((N, C, H, B), f32),
                pltpu.VMEM((steps, R, H, B), f32),
                pltpu.VMEM((steps, R - 1, H, B), f32),
                pltpu.VMEM((steps, R * C, lines, 1, K), f32),
                pltpu.VMEM((DEG, B), f32),
                node, node, node, node,
                dma((1,)),
                dma((1,)), dma((C,)),
                dma((1,)), dma((steps, C // 2)),
                dma((1,)), dma((steps,)),
                dma((1,)), dma((1,)), dma((N,)),
                dma((1,)), dma((steps,)),
                dma((1,)), dma((steps,)),
                dma((3,)),
            ],
            compiler_params=pltpu.CompilerParams(
                collective_id=0, has_side_effects=True, vmem_limit_bytes=40 * 1024 * 1024
            ),
        )(*(pltpu.with_memory_space_constraint(v, pltpu.HBM) for v in (tile_row, tile_col, label_class.reshape(1, B), tiles)))

    placed = (P(("row", "col"), None, None),) + (P(("row", "col")),) * 3
    return jax.shard_map(
        shards,
        mesh=mesh,
        in_specs=placed,
        out_specs=(P(("row", "col"), None), P(("row", "col"), None)),
        check_vma=False,
    )
```

```python
import functools

import jax
import jax.numpy as jnp
from jax import lax
from jax.experimental import pallas as pl
from jax.experimental.pallas import tpu as pltpu
from jax.sharding import PartitionSpec as P

CLASSES = 128
ITERS = 3
PAD = 16
DEG = 8
UNROLL = 32
PARTS = 4
CHAINS = 4
EARLY = 2
LIMIT = 32700.0
OFFSET = 2.4
NEAR, MID, FAR, READY, PERIOD, SUMS = 2.9, 3.9, 4.6, 5.5, 9.7, 5.0


def flip(index, mask):
    bit = 1
    result = index
    while bit <= mask:
        if mask & bit:
            result = result + bit * (1 - 2 * lax.rem(lax.div(index, bit), 2))
        bit *= 2
    return result


def kernel(
    R, C, row_hbm, col_hbm, label_hbm, tiles_hbm, out,
    tile_row, tile_col, pos, label_ref,
    tiles, lab, hot, acc0, rs0, deg, code, unit, panel, rep_r, rep_p, acc, rs, st,
    degree, direction, image, residual, answer,
    tile_sem, lab_send, lab_recv, code_send, code_recv, unit_send, unit_recv, side_send, side_recv, deg_send, deg_recv, rs0_send, rs0_recv, rs_send, rs_recv,
    st_send, st_recv, in_sem,
):
    T, B = tiles_hbm.shape[0], tiles_hbm.shape[1]
    Z = C // 2
    K, H = CLASSES, CLASSES // CHAINS
    Q = K // H
    G = H // 2
    f32, bf16, i32 = jnp.float32, jnp.bfloat16, jnp.int32
    unroll = R * C <= UNROLL
    row, col = lax.axis_index("row"), lax.axis_index("col")
    core = lax.rem(col, 2)
    chip = lax.div(col, 2)
    peer = col + 1 - 2 * core
    assert C % 2 == 0 and C & (C - 1) == 0 and R & (R - 1) == 0

    def col_partner(m):
        return flip(col, m)

    def row_partner(m):
        return flip(row, m)

    def loop(count, body, carry):
        if unroll:
            for n in range(count):
                carry = body(n, carry)
            return carry
        return lax.fori_loop(0, count, body, carry)

    inputs = [
        pltpu.make_async_copy(source, target, in_sem.at[n])
        for n, (source, target) in enumerate(
            [(label_hbm, label_ref), (row_hbm, tile_row), (col_hbm, tile_col)]
        )
    ]
    for cp in inputs:
        cp.start()
    barrier = pltpu.get_barrier_semaphore()
    for m in range(C - 1, 0, -1):
        pl.semaphore_signal(
            barrier, inc=1, device_id={"col": col_partner(m)}, device_id_type=pl.DeviceIdType.MESH
        )
    for m in range(R - 1, 0, -1):
        pl.semaphore_signal(
            barrier, inc=1, device_id={"row": row_partner(m)}, device_id_type=pl.DeviceIdType.MESH
        )
    step = -(-T // PARTS)
    for p in range(PARTS):
        lo, hi = p * step, min(T, (p + 1) * step)
        if lo < hi:
            pltpu.make_async_copy(
                tiles_hbm.at[pl.ds(lo, hi - lo)], tiles.at[pl.ds(lo, hi - lo)], tile_sem.at[0]
            ).start()
    if tiles.shape[0] > T:
        tiles[T] = jnp.zeros((B, B), bf16)
    inputs[0].wait()
    mine = label_ref[...]
    lab[col] = mine

    pl.semaphore_wait(barrier, C - 1 + R - 1)

    def send(src, dst, send_sem, recv_sem, where):
        pltpu.make_async_remote_copy(
            src_ref=src, dst_ref=dst, send_sem=send_sem, recv_sem=recv_sem,
            device_id=where, device_id_type=pl.DeviceIdType.MESH,
        ).start()

    def landed(ref, recv_sem):
        pltpu.make_async_remote_copy(
            src_ref=ref, dst_ref=ref, send_sem=tile_sem.at[0], recv_sem=recv_sem,
            device_id={"col": peer}, device_id_type=pl.DeviceIdType.MESH,
        ).wait_recv()

    def drained(ref, send_sem):
        pltpu.make_async_remote_copy(
            src_ref=ref, dst_ref=ref, send_sem=send_sem, recv_sem=tile_sem.at[0],
            device_id={"col": peer}, device_id_type=pl.DeviceIdType.MESH,
        ).wait_send()

    def other_chip(j):
        upper = lax.div(2 * chip, Z)
        low = chip + upper * (Z - 1 - 2 * chip)
        far = Z - 1 - j - lax.div(low + j + 1, Z)
        return far + upper * (Z - 1 - 2 * far)

    def tile_at(source, k):
        return tiles[pos[source * R + k]]

    def fold(product):
        folded = product[:, :K]
        for lane in range(K, B, K):
            folded = folded + product[:, lane : lane + K]
        return folded

    def sums_row(products):
        rows = []
        for lo in range(0, len(products), Q):
            part = [fold(p) for p in products[lo : lo + Q]]
            if len(part) < Q:
                part.append(jnp.zeros((K - H * len(part), K), f32))
            rows.append(jnp.sum(jnp.concatenate(part, axis=0).T, axis=0, keepdims=True))
        return rows

    def spread(rows, count):
        values = []
        for q in range(count):
            if q % Q == 0:
                square = jnp.broadcast_to(rows[q // Q], (K, K)).T
            values.append(square[q % Q * H : (q % Q + 1) * H])
        return values

    def wide(value):
        return jnp.concatenate([value] * (B // K), axis=1)

    def encode(t, value):
        top = jnp.clip(jnp.max(jnp.abs(value), axis=0, keepdims=True), 2.0**-100, 2.0**120)
        power = jnp.ceil(jnp.log2(top))
        whole = jnp.round(value * (jnp.exp2(-power) * LIMIT)).astype(i32)
        code[t, col] = (whole[:G] << 16) | (whole[G:] & 0xFFFF)
        unit[t, col] = jnp.exp2(power) * (1.0 / LIMIT)

    def decode(t, c):
        word = code[t, c]
        scale = unit[t, c]
        high = (word >> 16).astype(f32) * scale
        low = ((word << 16) >> 16).astype(f32) * scale
        return jnp.concatenate([high, low], axis=0)

    bounds = [0, min(2, C), min(6, C), C]

    def level(m):
        return sum(m >= bound for bound in bounds[1:])

    for m in range(C - 1, 0, -1):
        send(lab.at[col], lab.at[col], lab_send.at[0], lab_recv.at[level(m)], {"col": col_partner(m)})
    for cp in inputs[1:]:
        cp.wait()

    def place(n, carry):
        tile_row[n] = lax.rem(tile_row[n], C) * R + lax.div(tile_col[n], C)
        return carry

    lax.fori_loop(0, T, place, 0)
    miss = tiles.shape[0] - 1

    def locate(slot, carry):
        found = miss
        for n in range(T):
            found = jnp.minimum(found, jnp.where(tile_row[n] == slot, n, miss))
        pos[slot] = found
        return carry

    lax.fori_loop(0, R * C, locate, 0)
    class_axis = lax.broadcasted_iota(i32, (K, B), 0)
    ones = jnp.ones((PAD, B), bf16)

    def show(c):
        value = jnp.where(lab[c] == class_axis, 1.0, 0.0).astype(bf16)
        hot[c] = jnp.concatenate([ones, value], axis=0)

    show(col)
    free = jnp.broadcast_to(mine, (H, B)) < 0
    pltpu.make_async_copy(tiles, tiles, tile_sem.at[0]).wait() if tiles.shape[0] == T else pltpu.make_async_copy(
        tiles.at[pl.ds(0, T)], tiles.at[pl.ds(0, T)], tile_sem.at[0]
    ).wait()

    for group, (lo, hi) in enumerate(zip(bounds, bounds[1:])):
        if hi > max(lo, 1):
            landed(lab.at[pl.ds(0, hi - max(lo, 1))], lab_recv.at[group])
        for m in range(max(lo, 1), hi):
            show(col_partner(m))
        if hi > lo:
            for m in range(R - 1, -1, -1):
                k = row_partner(m)
                value = None if lo == 0 else acc0[k]
                for n in range(lo, hi):
                    c = col_partner(n) if n else col
                    part = jnp.dot(hot[c], tile_at(c, k), preferred_element_type=f32)
                    value = part if value is None else value + part
                acc0[k] = value

    for h in range(CHAINS):
        for m in range(R - 1, 0, -1):
            k = row_partner(m)
            send(acc0.at[k, pl.ds(PAD + h * H, H)], rs0.at[h, m - 1], rs0_send.at[0], rs0_recv.at[h], {"row": k})
    for m in range(R - 1, 0, -1):
        k = row_partner(m)
        send(acc0.at[k, pl.ds(PAD - DEG, DEG)], deg.at[m - 1], deg_send.at[0], deg_recv.at[0], {"row": k})

    lead = CHAINS - EARLY

    def slot(t):
        return t // ITERS * 2 + t % ITERS % 2

    def gather_start(t):
        early = t // ITERS >= lead
        own = code.at[t, col]
        for j in range(Z - 1):
            send(own, own, code_send.at[0], code_recv.at[slot(t), chip], {"col": 2 * other_chip(j) + core})
        send(own, own, code_send.at[0], code_recv.at[slot(t), chip], {"col": peer})
        if early:
            for m in range(R - 1, 0, -1):
                send(own, code.at[t, C + row], side_send.at[0], side_recv.at[slot(t - lead * ITERS)], {"row": row_partner(m)})
        own = unit.at[t, col]
        for m in range(C - 1, 0, -1):
            send(own, own, unit_send.at[0], unit_recv.at[slot(t)], {"col": col_partner(m)})
        if early:
            for m in range(R - 1, 0, -1):
                send(own, unit.at[t, C + row], side_send.at[1], unit_recv.at[slot(t)], {"row": row_partner(m)})

    def gather_relay(t, j):
        z = other_chip(j)
        block = code.at[t, 2 * z + core]
        landed(block, code_recv.at[slot(t), z])
        send(block, block, code_send.at[0], code_recv.at[slot(t), chip], {"col": peer})

    def gather_end(t):
        landed(code.at[t, pl.ds(0, Z)], code_recv.at[slot(t), chip])
        if t // ITERS >= lead:
            landed(code.at[t, pl.ds(0, R - 1)], side_recv.at[slot(t - lead * ITERS)])
            landed(unit.at[t, pl.ds(0, C + R - 2)], unit_recv.at[slot(t)])
        else:
            landed(unit.at[t, pl.ds(0, C - 1)], unit_recv.at[slot(t)])

    me = row * C + col

    def stats_start(t, rows):
        for i in range(st.shape[2]):
            st[t, me, i] = rows[i] if i < len(rows) else jnp.zeros((1, K), f32)
        own = st.at[t, me]

        def out(n, carry):
            other = lax.rem(me + n + 1, R * C)
            send(own, own, st_send.at[0], st_recv.at[slot(t)], {"row": lax.div(other, C), "col": lax.rem(other, C)})
            return carry

        if unroll:
            pairs = [(y, z) for y in range(R) for z in range(C)][1:]
            for y, z in sorted(pairs, key=lambda pair: -(pair[0].bit_count() + pair[1] // 2)):
                send(own, own, st_send.at[0], st_recv.at[slot(t)], {"row": row_partner(y), "col": col_partner(z)})
        else:
            lax.fori_loop(0, R * C - 1, out, 0)

    def stats_end(t):
        landed(st.at[t, pl.ds(0, R * C - 1)], st_recv.at[slot(t)])
        return jnp.sum(st[t], axis=0)

    def weigh():
        landed(deg, deg_recv.at[0])
        value = acc0[row, PAD - DEG : PAD]
        for m in range(1, R):
            value = value + deg[m - 1]
        degree[...] = value

    def apply(t, d):
        mixed = acc[t, row]
        for m in range(1, R):
            mixed = mixed + rs[t, m - 1]
        return jnp.where(free, degree[0:1] * d - mixed, d)

    def chain(h):
        clock = OFFSET * h
        yield clock
        landed(rs0.at[h], rs0_recv.at[h])
        value = acc0[row, PAD + h * H : PAD + (h + 1) * H]
        for m in range(1, R):
            value = value + rs0[h, m - 1]
        rhs = jnp.where(free, value, 0.0)
        encode(h * ITERS, rhs)
        gather_start(h * ITERS)
        answer[h] = jnp.zeros((H, B), f32)
        residual[h] = rhs
        direction[h] = rhs
        norm = None
        for s in range(ITERS):
            t = h * ITERS + s
            last = s + 1 == ITERS
            if Z > 1:
                yield clock + NEAR
                gather_relay(t, Z - 2)
            if Z > 2:
                yield clock + MID
                for j in range(Z - 3, 0, -1):
                    gather_relay(t, j)
                yield clock + FAR
                gather_relay(t, 0)
            yield clock + READY
            if s:
                total = stats_end(t - 1)
                if s == 1:
                    di, ii, norm = spread(total, 3)
                    ri = di
                else:
                    di, ri, ii = spread(total, 3)
                alpha = norm / di
                after = norm - 2.0 * alpha * ri + alpha * alpha * ii
                beta = after / norm
                norm = after
                a, b = wide(alpha), wide(beta)
            gather_end(t)

            def refresh(c, carry, side=False):
                fresh = decode(t, c)
                if s == 0:
                    rep_r[h, c] = fresh
                else:
                    old = rep_r[h, c]
                    r = old - a * fresh
                    p = r + b * (old if s == 1 else rep_p[h, c])
                    if not last:
                        rep_r[h, c] = r
                    if side or not last:
                        rep_p[h, c] = p
                    fresh = p
                if not side:
                    panel[h, c] = fresh.astype(bf16)
                return carry

            loop(C, refresh, 0)

            def ship(m, k, value):
                acc[t, k] = value
                if m:
                    send(acc.at[t, k], rs.at[t, m - 1], rs_send.at[0], rs_recv.at[t // ITERS], {"row": k})

            held = None
            for m in range(R - 1, -1, -1):
                k = row_partner(m)

                def one(c, value):
                    part = jnp.dot(panel[h, c], tile_at(c, k), preferred_element_type=f32)
                    return part if value is None else value + part

                value = loop(C, one, None if unroll else jnp.zeros((H, B), f32))
                if held is not None:
                    ship(*held)
                held = (m, k, value)
            ship(*held)
            for m in range(1, R if h >= lead else 1):
                refresh(C + row_partner(m), 0, True)
            if s:
                d = direction[h]
                r = residual[h] - a * image[h]
                answer[h] = answer[h] + a * d
                residual[h] = r
                direction[h] = r + b * d
            if last and h >= lead:
                d = direction[h]
                inner = jnp.where(free, degree[0:1] * d, d) * d - d * acc[t, row]
                for m in range(1, R):
                    k = row_partner(m)
                    inner = inner - rep_p[h, C + k] * acc[t, k]
                stats_start(t, sums_row([inner]))
                break
            clock += PERIOD
            yield clock
            if h == 0 and s == 0:
                weigh()
            landed(rs.at[t], rs_recv.at[t // ITERS])
            i = apply(t, direction[h])
            image[h] = i
            d, r = direction[h], residual[h]
            if last:
                stats_start(t, sums_row([d * i]))
                break
            encode(t + 1, i)
            gather_start(t + 1)
            stats_start(t, sums_row([d * i, i * i, r * r] if s == 0 else [d * i, r * i, i * i]))
        d = direction[h]
        if h >= lead:
            yield clock + READY + SUMS
            landed(rs.at[t], rs_recv.at[t // ITERS])
            i = apply(t, d)
        else:
            yield clock + SUMS
            i = image[h]
        (di,) = spread(stats_end(t), 1)
        a = wide(norm / di)
        out[0:B, h * H : (h + 1) * H] = ((8.0 * K) * (answer[h] + a * d)).T
        out[B : 2 * B, h * H : (h + 1) * H] = (residual[h] - a * i).T

    queue = []
    for h in range(CHAINS):
        one = chain(h)
        queue.append((next(one), h, one))
    while queue:
        queue.sort(key=lambda entry: entry[:2])
        _, h, one = queue.pop(0)
        when = next(one, None)
        if when is not None:
            queue.append((when, h, one))

    drained(lab.at[pl.ds(0, C - 1)], lab_send.at[0])
    drained(code.at[:, pl.ds(0, C - 1)], code_send.at[0])
    drained(unit.at[:, pl.ds(0, C - 1)], unit_send.at[0])
    if EARLY:
        drained(code.at[pl.ds(0, EARLY * ITERS), pl.ds(0, R - 1)], side_send.at[0])
        drained(unit.at[pl.ds(0, EARLY * ITERS), pl.ds(0, R - 1)], side_send.at[1])
    drained(deg, deg_send.at[0])
    drained(rs0, rs0_send.at[0])
    drained(rs, rs_send.at[0])
    drained(st.at[:, pl.ds(0, R * C - 1)], st_send.at[0])


def solution(mesh):
    R, C = mesh.shape["row"], mesh.shape["col"]

    def shards(tiles, tile_row, tile_col, label_class):
        T, B = tiles.shape[0], tiles.shape[1]
        K, H, N = CLASSES, CLASSES // CHAINS, CHAINS
        held = T if T == R * C else T + 1
        f32, bf16, i32 = jnp.float32, jnp.bfloat16, jnp.int32
        dma = pltpu.SemaphoreType.DMA
        vmem, hbm = pl.BlockSpec(memory_space=pltpu.VMEM), pl.BlockSpec(memory_space=pltpu.HBM)
        smem = pltpu.SMEM
        node = pltpu.VMEM((N, H, B), f32)
        steps = N * ITERS
        lines = -(-3 // (K // H))
        both = pl.pallas_call(
            functools.partial(kernel, R, C),
            out_shape=jax.ShapeDtypeStruct((2 * B, K), f32),
            in_specs=[
                hbm, hbm, hbm, hbm,
            ],
            out_specs=vmem,
            scratch_shapes=[
                smem((T,), i32), smem((T,), i32), smem((R * C,), i32), pltpu.VMEM((1, B), i32),
                pltpu.VMEM((held, B, B), bf16),
                pltpu.VMEM((C, 1, B), i32),
                pltpu.VMEM((C, PAD + K, B), bf16),
                pltpu.VMEM((R, PAD + K, B), f32),
                pltpu.VMEM((N, R - 1, H, B), f32),
                pltpu.VMEM((R - 1, DEG, B), f32),
                pltpu.VMEM((steps, C + R, H // 2, B), i32),
                pltpu.VMEM((steps, C + R, 1, B), f32),
                pltpu.VMEM((N, C, H, B), bf16),
                pltpu.VMEM((N, C + R, H, B), f32),
                pltpu.VMEM((N, C + R, H, B), f32),
                pltpu.VMEM((steps, R, H, B), f32),
                pltpu.VMEM((steps, R - 1, H, B), f32),
                pltpu.VMEM((steps, R * C, lines, 1, K), f32),
                pltpu.VMEM((DEG, B), f32),
                node, node, node, node,
                dma((1,)),
                dma((1,)), dma((3,)),
                dma((1,)), dma((2 * N, C // 2)),
                dma((1,)), dma((2 * N,)), dma((2,)), dma((2 * max(EARLY, 1),)),
                dma((1,)), dma((1,)), dma((1,)), dma((N,)),
                dma((1,)), dma((N,)),
                dma((1,)), dma((2 * N,)),
                dma((3,)),
            ],
            compiler_params=pltpu.CompilerParams(
                collective_id=0, has_side_effects=True, vmem_limit_bytes=40 * 1024 * 1024
            ),
        )(*(pltpu.with_memory_space_constraint(v, pltpu.HBM) for v in (tile_row, tile_col, label_class.reshape(1, B), tiles)))
        return both[:B], both[B:]

    placed = (P(("row", "col"), None, None),) + (P(("row", "col")),) * 3
    return jax.shard_map(
        shards,
        mesh=mesh,
        in_specs=placed,
        out_specs=(P(("row", "col"), None), P(("row", "col"), None)),
        check_vma=False,
    )
```

```python
import functools

import jax
import jax.numpy as jnp
from jax import lax
from jax.experimental import pallas as pl
from jax.experimental.pallas import tpu as pltpu
from jax.sharding import PartitionSpec as P

CLASSES = 128
ITERS = 3
PAD = 16
DEG = 8
UNROLL = 32
PARTS = 4
CHAINS = 4
EARLY = 2
LIMIT = 32700.0
OFFSET = 2.4
NEAR, MID, FAR, READY, PERIOD, SUMS = 2.9, 3.9, 4.4, 4.9, 9.3, 4.5


def flip(index, mask):
    bit = 1
    result = index
    while bit <= mask:
        if mask & bit:
            result = result + bit * (1 - 2 * lax.rem(lax.div(index, bit), 2))
        bit *= 2
    return result


def kernel(
    R, C, row_hbm, col_hbm, label_hbm, tiles_hbm, out,
    tile_row, tile_col, pos, label_ref,
    tiles, lab, hot, acc0, rs0, deg, code, unit, panel, rep_r, rep_p, acc, piece, grade, rs, rg, st,
    degree, direction, image, residual, answer,
    tile_sem, lab_send, lab_recv, code_send, code_recv, unit_send, unit_recv, side_send, side_recv, deg_send, deg_recv, rs0_send, rs0_recv, rs_send, rs_recv, rg_send, rg_recv,
    st_send, st_recv, in_sem,
):
    T, B = tiles_hbm.shape[0], tiles_hbm.shape[1]
    Z = C // 2
    K, H = CLASSES, CLASSES // CHAINS
    Q = K // H
    G = H // 2
    f32, bf16, i32 = jnp.float32, jnp.bfloat16, jnp.int32
    unroll = R * C <= UNROLL
    row, col = lax.axis_index("row"), lax.axis_index("col")
    core = lax.rem(col, 2)
    chip = lax.div(col, 2)
    peer = col + 1 - 2 * core
    assert C % 2 == 0 and C & (C - 1) == 0 and R & (R - 1) == 0

    def col_partner(m):
        return flip(col, m)

    def row_partner(m):
        return flip(row, m)

    def loop(count, body, carry):
        if unroll:
            for n in range(count):
                carry = body(n, carry)
            return carry
        return lax.fori_loop(0, count, body, carry)

    inputs = [
        pltpu.make_async_copy(source, target, in_sem.at[n])
        for n, (source, target) in enumerate(
            [(label_hbm, label_ref), (row_hbm, tile_row), (col_hbm, tile_col)]
        )
    ]
    for cp in inputs:
        cp.start()
    barrier = pltpu.get_barrier_semaphore()
    for m in range(C - 1, 0, -1):
        pl.semaphore_signal(
            barrier, inc=1, device_id={"col": col_partner(m)}, device_id_type=pl.DeviceIdType.MESH
        )
    for m in range(R - 1, 0, -1):
        pl.semaphore_signal(
            barrier, inc=1, device_id={"row": row_partner(m)}, device_id_type=pl.DeviceIdType.MESH
        )
    step = -(-T // PARTS)
    for p in range(PARTS):
        lo, hi = p * step, min(T, (p + 1) * step)
        if lo < hi:
            pltpu.make_async_copy(
                tiles_hbm.at[pl.ds(lo, hi - lo)], tiles.at[pl.ds(lo, hi - lo)], tile_sem.at[0]
            ).start()
    if tiles.shape[0] > T:
        tiles[T] = jnp.zeros((B, B), bf16)
    inputs[0].wait()
    mine = label_ref[...]
    lab[col] = mine

    pl.semaphore_wait(barrier, C - 1 + R - 1)

    def send(src, dst, send_sem, recv_sem, where):
        pltpu.make_async_remote_copy(
            src_ref=src, dst_ref=dst, send_sem=send_sem, recv_sem=recv_sem,
            device_id=where, device_id_type=pl.DeviceIdType.MESH,
        ).start()

    def landed(ref, recv_sem):
        pltpu.make_async_remote_copy(
            src_ref=ref, dst_ref=ref, send_sem=tile_sem.at[0], recv_sem=recv_sem,
            device_id={"col": peer}, device_id_type=pl.DeviceIdType.MESH,
        ).wait_recv()

    def drained(ref, send_sem):
        pltpu.make_async_remote_copy(
            src_ref=ref, dst_ref=ref, send_sem=send_sem, recv_sem=tile_sem.at[0],
            device_id={"col": peer}, device_id_type=pl.DeviceIdType.MESH,
        ).wait_send()

    def other_chip(j):
        upper = lax.div(2 * chip, Z)
        low = chip + upper * (Z - 1 - 2 * chip)
        far = Z - 1 - j - lax.div(low + j + 1, Z)
        return far + upper * (Z - 1 - 2 * far)

    def tile_at(source, k):
        return tiles[pos[source * R + k]]

    def fold(product):
        folded = product[:, :K]
        for lane in range(K, B, K):
            folded = folded + product[:, lane : lane + K]
        return folded

    def sums_row(products):
        rows = []
        for lo in range(0, len(products), Q):
            part = [fold(p) for p in products[lo : lo + Q]]
            if len(part) < Q:
                part.append(jnp.zeros((K - H * len(part), K), f32))
            rows.append(jnp.sum(jnp.concatenate(part, axis=0).T, axis=0, keepdims=True))
        return rows

    def spread(rows, count):
        values = []
        for q in range(count):
            if q % Q == 0:
                square = jnp.broadcast_to(rows[q // Q], (K, K)).T
            values.append(square[q % Q * H : (q % Q + 1) * H])
        return values

    def wide(value):
        return jnp.concatenate([value] * (B // K), axis=1)

    def pack(value):
        top = jnp.clip(jnp.max(jnp.abs(value), axis=0, keepdims=True), 2.0**-100, 2.0**120)
        power = jnp.ceil(jnp.log2(top))
        whole = jnp.round(value * (jnp.exp2(-power) * LIMIT)).astype(i32)
        return (whole[:G] << 16) | (whole[G:] & 0xFFFF), jnp.exp2(power) * (1.0 / LIMIT)

    def encode(t, value):
        code[t, col], unit[t, col] = pack(value)

    def decode(t, c):
        return unpack(code[t, c], unit[t, c])

    def unpack(word, scale):
        high = (word >> 16).astype(f32) * scale
        low = ((word << 16) >> 16).astype(f32) * scale
        return jnp.concatenate([high, low], axis=0)

    bounds = [0, min(2, C), min(6, C), C]

    def level(m):
        return sum(m >= bound for bound in bounds[1:])

    for m in range(C - 1, 0, -1):
        send(lab.at[col], lab.at[col], lab_send.at[0], lab_recv.at[level(m)], {"col": col_partner(m)})
    for cp in inputs[1:]:
        cp.wait()

    def place(n, carry):
        tile_row[n] = lax.rem(tile_row[n], C) * R + lax.div(tile_col[n], C)
        return carry

    lax.fori_loop(0, T, place, 0)
    miss = tiles.shape[0] - 1

    def locate(slot, carry):
        found = miss
        for n in range(T):
            found = jnp.minimum(found, jnp.where(tile_row[n] == slot, n, miss))
        pos[slot] = found
        return carry

    lax.fori_loop(0, R * C, locate, 0)
    class_axis = lax.broadcasted_iota(i32, (K, B), 0)
    ones = jnp.ones((PAD, B), bf16)

    def show(c):
        value = jnp.where(lab[c] == class_axis, 1.0, 0.0).astype(bf16)
        hot[c] = jnp.concatenate([ones, value], axis=0)

    show(col)
    free = jnp.broadcast_to(mine, (H, B)) < 0
    pltpu.make_async_copy(tiles, tiles, tile_sem.at[0]).wait() if tiles.shape[0] == T else pltpu.make_async_copy(
        tiles.at[pl.ds(0, T)], tiles.at[pl.ds(0, T)], tile_sem.at[0]
    ).wait()

    for group, (lo, hi) in enumerate(zip(bounds, bounds[1:])):
        if hi > max(lo, 1):
            landed(lab.at[pl.ds(0, hi - max(lo, 1))], lab_recv.at[group])
        for m in range(max(lo, 1), hi):
            show(col_partner(m))
        if hi > lo:
            for m in range(R - 1, -1, -1):
                k = row_partner(m)
                value = None if lo == 0 else acc0[k]
                for n in range(lo, hi):
                    c = col_partner(n) if n else col
                    part = jnp.dot(hot[c], tile_at(c, k), preferred_element_type=f32)
                    value = part if value is None else value + part
                acc0[k] = value

    for h in range(CHAINS):
        for m in range(R - 1, 0, -1):
            k = row_partner(m)
            send(acc0.at[k, pl.ds(PAD + h * H, H)], rs0.at[h, m - 1], rs0_send.at[0], rs0_recv.at[h], {"row": k})
    for m in range(R - 1, 0, -1):
        k = row_partner(m)
        send(acc0.at[k, pl.ds(PAD - DEG, DEG)], deg.at[m - 1], deg_send.at[0], deg_recv.at[0], {"row": k})

    lead = CHAINS - EARLY

    def slot(t):
        return t // ITERS * 2 + t % ITERS % 2

    def gather_start(t):
        early = t // ITERS >= lead
        own = code.at[t, col]
        for j in range(Z - 1):
            send(own, own, code_send.at[0], code_recv.at[slot(t), chip], {"col": 2 * other_chip(j) + core})
        send(own, own, code_send.at[0], code_recv.at[slot(t), chip], {"col": peer})
        if early:
            for m in range(R - 1, 0, -1):
                send(own, code.at[t, C + row], side_send.at[0], side_recv.at[slot(t - lead * ITERS)], {"row": row_partner(m)})
        own = unit.at[t, col]
        for m in range(C - 1, 0, -1):
            send(own, own, unit_send.at[0], unit_recv.at[slot(t)], {"col": col_partner(m)})
        if early:
            for m in range(R - 1, 0, -1):
                send(own, unit.at[t, C + row], side_send.at[1], unit_recv.at[slot(t)], {"row": row_partner(m)})

    def gather_relay(t, j):
        z = other_chip(j)
        block = code.at[t, 2 * z + core]
        landed(block, code_recv.at[slot(t), z])
        send(block, block, code_send.at[0], code_recv.at[slot(t), chip], {"col": peer})

    def gather_end(t):
        landed(code.at[t, pl.ds(0, Z)], code_recv.at[slot(t), chip])
        if t // ITERS >= lead:
            landed(code.at[t, pl.ds(0, R - 1)], side_recv.at[slot(t - lead * ITERS)])
            landed(unit.at[t, pl.ds(0, C + R - 2)], unit_recv.at[slot(t)])
        else:
            landed(unit.at[t, pl.ds(0, C - 1)], unit_recv.at[slot(t)])

    me = row * C + col

    def stats_start(t, rows):
        for i in range(st.shape[2]):
            st[t, me, i] = rows[i] if i < len(rows) else jnp.zeros((1, K), f32)
        own = st.at[t, me]

        def out(n, carry):
            other = lax.rem(me + n + 1, R * C)
            send(own, own, st_send.at[0], st_recv.at[slot(t)], {"row": lax.div(other, C), "col": lax.rem(other, C)})
            return carry

        if unroll:
            pairs = [(y, z) for y in range(R) for z in range(C)][1:]
            for y, z in sorted(pairs, key=lambda pair: -(pair[0].bit_count() + pair[1] // 2)):
                send(own, own, st_send.at[0], st_recv.at[slot(t)], {"row": row_partner(y), "col": col_partner(z)})
        else:
            lax.fori_loop(0, R * C - 1, out, 0)

    def stats_end(t):
        landed(st.at[t, pl.ds(0, R * C - 1)], st_recv.at[slot(t)])
        return jnp.sum(st[t], axis=0)

    def weigh():
        landed(deg, deg_recv.at[0])
        value = acc0[row, PAD - DEG : PAD]
        for m in range(1, R):
            value = value + deg[m - 1]
        degree[...] = value

    def apply(t, d):
        mixed = acc[t // ITERS, row]
        for m in range(1, R):
            mixed = mixed + unpack(rs[t, m - 1], rg[t, m - 1])
        return jnp.where(free, degree[0:1] * d - mixed, d)

    def chain(h):
        clock = OFFSET * h
        yield clock
        landed(rs0.at[h], rs0_recv.at[h])
        value = acc0[row, PAD + h * H : PAD + (h + 1) * H]
        for m in range(1, R):
            value = value + rs0[h, m - 1]
        rhs = jnp.where(free, value, 0.0)
        encode(h * ITERS, rhs)
        gather_start(h * ITERS)
        answer[h] = jnp.zeros((H, B), f32)
        residual[h] = rhs
        direction[h] = rhs
        norm = None
        for s in range(ITERS):
            t = h * ITERS + s
            last = s + 1 == ITERS
            if Z > 1:
                yield clock + NEAR
                gather_relay(t, Z - 2)
            if Z > 2:
                yield clock + MID
                for j in range(Z - 3, 0, -1):
                    gather_relay(t, j)
                yield clock + FAR
                gather_relay(t, 0)
            yield clock + READY
            if s:
                total = stats_end(t - 1)
                if s == 1:
                    di, ii, norm = spread(total, 3)
                    ri = di
                else:
                    di, ri, ii = spread(total, 3)
                alpha = norm / di
                after = norm - 2.0 * alpha * ri + alpha * alpha * ii
                beta = after / norm
                norm = after
                a, b = wide(alpha), wide(beta)
            gather_end(t)

            def refresh(c, carry, side=False):
                fresh = decode(t, c)
                if s == 0:
                    rep_r[h, c] = fresh
                else:
                    old = rep_r[h, c]
                    r = old - a * fresh
                    p = r + b * (old if s == 1 else rep_p[h, c])
                    if not last:
                        rep_r[h, c] = r
                    if side or not last:
                        rep_p[h, c] = p
                    fresh = p
                if not side:
                    panel[h, c] = fresh.astype(bf16)
                return carry

            loop(C, refresh, 0)

            def ship(m, k, value):
                if m == 0 or (last and h >= lead):
                    acc[h, k] = value
                if m:
                    piece[t, k], grade[t, k] = pack(value)
                    send(piece.at[t, k], rs.at[t, m - 1], rs_send.at[0], rs_recv.at[h], {"row": k})
                    send(grade.at[t, k], rg.at[t, m - 1], rg_send.at[0], rg_recv.at[h], {"row": k})

            held = None
            for m in range(R - 1, -1, -1):
                k = row_partner(m)

                def one(c, value):
                    part = jnp.dot(panel[h, c], tile_at(c, k), preferred_element_type=f32)
                    return part if value is None else value + part

                value = loop(C, one, None if unroll else jnp.zeros((H, B), f32))
                if held is not None:
                    ship(*held)
                held = (m, k, value)
            ship(*held)
            for m in range(1, R if h >= lead else 1):
                refresh(C + row_partner(m), 0, True)
            if s:
                d = direction[h]
                r = residual[h] - a * image[h]
                answer[h] = answer[h] + a * d
                residual[h] = r
                direction[h] = r + b * d
            if last and h >= lead:
                d = direction[h]
                inner = jnp.where(free, degree[0:1] * d, d) * d - d * acc[h, row]
                for m in range(1, R):
                    k = row_partner(m)
                    inner = inner - rep_p[h, C + k] * acc[h, k]
                stats_start(t, sums_row([inner]))
                break
            clock += PERIOD
            yield clock
            if h == 0 and s == 0:
                weigh()
            landed(rs.at[t], rs_recv.at[h])
            landed(rg.at[t], rg_recv.at[h])
            i = apply(t, direction[h])
            image[h] = i
            d, r = direction[h], residual[h]
            if last:
                stats_start(t, sums_row([d * i]))
                break
            encode(t + 1, i)
            gather_start(t + 1)
            stats_start(t, sums_row([d * i, i * i, r * r] if s == 0 else [d * i, r * i, i * i]))
        d = direction[h]
        if h >= lead:
            yield clock + READY + SUMS
            landed(rs.at[t], rs_recv.at[h])
            landed(rg.at[t], rg_recv.at[h])
            i = apply(t, d)
        else:
            yield clock + SUMS
            i = image[h]
        (di,) = spread(stats_end(t), 1)
        a = wide(norm / di)
        out[0:B, h * H : (h + 1) * H] = ((8.0 * K) * (answer[h] + a * d)).T
        out[B : 2 * B, h * H : (h + 1) * H] = (residual[h] - a * i).T

    queue = []
    for h in range(CHAINS):
        one = chain(h)
        queue.append((next(one), h, one))
    while queue:
        queue.sort(key=lambda entry: entry[:2])
        _, h, one = queue.pop(0)
        when = next(one, None)
        if when is not None:
            queue.append((when, h, one))

    drained(lab.at[pl.ds(0, C - 1)], lab_send.at[0])
    drained(code.at[:, pl.ds(0, C - 1)], code_send.at[0])
    drained(unit.at[:, pl.ds(0, C - 1)], unit_send.at[0])
    if EARLY:
        drained(code.at[pl.ds(0, EARLY * ITERS), pl.ds(0, R - 1)], side_send.at[0])
        drained(unit.at[pl.ds(0, EARLY * ITERS), pl.ds(0, R - 1)], side_send.at[1])
    drained(deg, deg_send.at[0])
    drained(rs0, rs0_send.at[0])
    drained(rs, rs_send.at[0])
    drained(rg, rg_send.at[0])
    drained(st.at[:, pl.ds(0, R * C - 1)], st_send.at[0])


def solution(mesh):
    R, C = mesh.shape["row"], mesh.shape["col"]

    def shards(tiles, tile_row, tile_col, label_class):
        T, B = tiles.shape[0], tiles.shape[1]
        K, H, N = CLASSES, CLASSES // CHAINS, CHAINS
        held = T if T == R * C else T + 1
        f32, bf16, i32 = jnp.float32, jnp.bfloat16, jnp.int32
        dma = pltpu.SemaphoreType.DMA
        vmem, hbm = pl.BlockSpec(memory_space=pltpu.VMEM), pl.BlockSpec(memory_space=pltpu.HBM)
        smem = pltpu.SMEM
        node = pltpu.VMEM((N, H, B), f32)
        steps = N * ITERS
        lines = -(-3 // (K // H))
        both = pl.pallas_call(
            functools.partial(kernel, R, C),
            out_shape=jax.ShapeDtypeStruct((2 * B, K), f32),
            in_specs=[
                hbm, hbm, hbm, hbm,
            ],
            out_specs=vmem,
            scratch_shapes=[
                smem((T,), i32), smem((T,), i32), smem((R * C,), i32), pltpu.VMEM((1, B), i32),
                pltpu.VMEM((held, B, B), bf16),
                pltpu.VMEM((C, 1, B), i32),
                pltpu.VMEM((C, PAD + K, B), bf16),
                pltpu.VMEM((R, PAD + K, B), f32),
                pltpu.VMEM((N, R - 1, H, B), f32),
                pltpu.VMEM((R - 1, DEG, B), f32),
                pltpu.VMEM((steps, C + R, H // 2, B), i32),
                pltpu.VMEM((steps, C + R, 1, B), f32),
                pltpu.VMEM((N, C, H, B), bf16),
                pltpu.VMEM((N, C + R, H, B), f32),
                pltpu.VMEM((N, C + R, H, B), f32),
                pltpu.VMEM((N, R, H, B), f32),
                pltpu.VMEM((steps, R, H // 2, B), i32),
                pltpu.VMEM((steps, R, 1, B), f32),
                pltpu.VMEM((steps, R - 1, H // 2, B), i32),
                pltpu.VMEM((steps, R - 1, 1, B), f32),
                pltpu.VMEM((steps, R * C, lines, 1, K), f32),
                pltpu.VMEM((DEG, B), f32),
                node, node, node, node,
                dma((1,)),
                dma((1,)), dma((3,)),
                dma((1,)), dma((2 * N, C // 2)),
                dma((1,)), dma((2 * N,)), dma((2,)), dma((2 * max(EARLY, 1),)),
                dma((1,)), dma((1,)), dma((1,)), dma((N,)),
                dma((1,)), dma((N,)), dma((1,)), dma((N,)),
                dma((1,)), dma((2 * N,)),
                dma((3,)),
            ],
            compiler_params=pltpu.CompilerParams(
                collective_id=0, has_side_effects=True, vmem_limit_bytes=40 * 1024 * 1024
            ),
        )(*(pltpu.with_memory_space_constraint(v, pltpu.HBM) for v in (tile_row, tile_col, label_class.reshape(1, B), tiles)))
        return both[:B], both[B:]

    placed = (P(("row", "col"), None, None),) + (P(("row", "col")),) * 3
    return jax.shard_map(
        shards,
        mesh=mesh,
        in_specs=placed,
        out_specs=(P(("row", "col"), None), P(("row", "col"), None)),
        check_vma=False,
    )
```

```python
import functools

import jax
import jax.numpy as jnp
from jax import lax
from jax.experimental import pallas as pl
from jax.experimental.pallas import tpu as pltpu
from jax.sharding import PartitionSpec as P

CLASSES = 128
ITERS = 3
PAD = 16
DEG = 8
UNROLL = 32
PARTS = 4
CHAINS = 4
EARLY = 2
LIMIT = 32700.0
OFFSET = 2.2
NEAR, MID, FAR, READY, PERIOD, SUMS = 2.9, 3.6, 4.3, 4.9, 8.8, 4.3


def flip(index, mask):
    bit = 1
    result = index
    while bit <= mask:
        if mask & bit:
            result = result + bit * (1 - 2 * lax.rem(lax.div(index, bit), 2))
        bit *= 2
    return result


def kernel(
    R, C, row_hbm, col_hbm, label_hbm, tiles_hbm, out,
    tile_row, tile_col, pos, label_ref,
    tiles, lab, hot, acc0, rs0, deg, code, unit, panel, rep_r, rep_p, acc, piece, grade, rs, rg, st,
    degree, direction, image, residual, answer,
    tile_sem, lab_send, lab_recv, code_send, code_recv, unit_send, unit_recv, side_send, side_recv, deg_send, deg_recv, rs0_send, rs0_recv, rs_send, rs_recv, rg_send, rg_recv,
    st_send, st_recv, in_sem,
):
    T, B = tiles_hbm.shape[0], tiles_hbm.shape[1]
    Z = C // 2
    K, H = CLASSES, CLASSES // CHAINS
    Q = K // H
    G = H // 2
    f32, bf16, i32 = jnp.float32, jnp.bfloat16, jnp.int32
    unroll = R * C <= UNROLL
    row, col = lax.axis_index("row"), lax.axis_index("col")
    core = lax.rem(col, 2)
    chip = lax.div(col, 2)
    peer = col + 1 - 2 * core
    assert C % 2 == 0 and C & (C - 1) == 0 and R & (R - 1) == 0

    def col_partner(m):
        return flip(col, m)

    def row_partner(m):
        return flip(row, m)

    def loop(count, body, carry):
        if unroll:
            for n in range(count):
                carry = body(n, carry)
            return carry
        return lax.fori_loop(0, count, body, carry)

    inputs = [
        pltpu.make_async_copy(source, target, in_sem.at[n])
        for n, (source, target) in enumerate(
            [(label_hbm, label_ref), (row_hbm, tile_row), (col_hbm, tile_col)]
        )
    ]
    for cp in inputs:
        cp.start()
    barrier = pltpu.get_barrier_semaphore()
    for m in range(C - 1, 0, -1):
        pl.semaphore_signal(
            barrier, inc=1, device_id={"col": col_partner(m)}, device_id_type=pl.DeviceIdType.MESH
        )
    for m in range(R - 1, 0, -1):
        pl.semaphore_signal(
            barrier, inc=1, device_id={"row": row_partner(m)}, device_id_type=pl.DeviceIdType.MESH
        )
    step = -(-T // PARTS)
    for p in range(PARTS):
        lo, hi = p * step, min(T, (p + 1) * step)
        if lo < hi:
            pltpu.make_async_copy(
                tiles_hbm.at[pl.ds(lo, hi - lo)], tiles.at[pl.ds(lo, hi - lo)], tile_sem.at[0]
            ).start()
    if tiles.shape[0] > T:
        tiles[T] = jnp.zeros((B, B), bf16)
    inputs[0].wait()
    mine = label_ref[...]
    lab[col] = mine

    pl.semaphore_wait(barrier, C - 1 + R - 1)

    def send(src, dst, send_sem, recv_sem, where):
        pltpu.make_async_remote_copy(
            src_ref=src, dst_ref=dst, send_sem=send_sem, recv_sem=recv_sem,
            device_id=where, device_id_type=pl.DeviceIdType.MESH,
        ).start()

    def landed(ref, recv_sem):
        pltpu.make_async_remote_copy(
            src_ref=ref, dst_ref=ref, send_sem=tile_sem.at[0], recv_sem=recv_sem,
            device_id={"col": peer}, device_id_type=pl.DeviceIdType.MESH,
        ).wait_recv()

    def drained(ref, send_sem):
        pltpu.make_async_remote_copy(
            src_ref=ref, dst_ref=ref, send_sem=send_sem, recv_sem=tile_sem.at[0],
            device_id={"col": peer}, device_id_type=pl.DeviceIdType.MESH,
        ).wait_send()

    def other_chip(j):
        upper = lax.div(2 * chip, Z)
        low = chip + upper * (Z - 1 - 2 * chip)
        far = Z - 1 - j - lax.div(low + j + 1, Z)
        return far + upper * (Z - 1 - 2 * far)

    def tile_at(source, k):
        return tiles[pos[source * R + k]]

    def fold(product):
        folded = product[:, :K]
        for lane in range(K, B, K):
            folded = folded + product[:, lane : lane + K]
        return folded

    def sums_row(products):
        rows = []
        for lo in range(0, len(products), Q):
            part = [fold(p) for p in products[lo : lo + Q]]
            if len(part) < Q:
                part.append(jnp.zeros((K - H * len(part), K), f32))
            rows.append(jnp.sum(jnp.concatenate(part, axis=0).T, axis=0, keepdims=True))
        return rows

    def spread(rows, count):
        values = []
        for q in range(count):
            if q % Q == 0:
                square = jnp.broadcast_to(rows[q // Q], (K, K)).T
            values.append(square[q % Q * H : (q % Q + 1) * H])
        return values

    def wide(value):
        return jnp.concatenate([value] * (B // K), axis=1)

    def pack(value):
        top = jnp.clip(jnp.max(jnp.abs(value), axis=0, keepdims=True), 2.0**-100, 2.0**120)
        power = jnp.ceil(jnp.log2(top))
        whole = jnp.round(value * (jnp.exp2(-power) * LIMIT)).astype(i32)
        return (whole[:G] << 16) | (whole[G:] & 0xFFFF), jnp.exp2(power) * (1.0 / LIMIT)

    def encode(t, value):
        code[t, col], unit[t, col] = pack(value)

    def decode(t, c):
        return unpack(code[t, c], unit[t, c])

    def unpack(word, scale):
        high = (word >> 16).astype(f32) * scale
        low = ((word << 16) >> 16).astype(f32) * scale
        return jnp.concatenate([high, low], axis=0)

    bounds = [0, min(2, C), min(6, C), C]

    def level(m):
        return sum(m >= bound for bound in bounds[1:])

    for m in range(C - 1, 0, -1):
        send(lab.at[col], lab.at[col], lab_send.at[0], lab_recv.at[level(m)], {"col": col_partner(m)})
    for cp in inputs[1:]:
        cp.wait()

    def place(n, carry):
        tile_row[n] = lax.rem(tile_row[n], C) * R + lax.div(tile_col[n], C)
        return carry

    lax.fori_loop(0, T, place, 0)
    miss = tiles.shape[0] - 1

    def locate(slot, carry):
        found = miss
        for n in range(T):
            found = jnp.minimum(found, jnp.where(tile_row[n] == slot, n, miss))
        pos[slot] = found
        return carry

    lax.fori_loop(0, R * C, locate, 0)
    class_axis = lax.broadcasted_iota(i32, (K, B), 0)
    ones = jnp.ones((PAD, B), bf16)

    def show(c):
        value = jnp.where(lab[c] == class_axis, 1.0, 0.0).astype(bf16)
        hot[c] = jnp.concatenate([ones, value], axis=0)

    show(col)
    free = jnp.broadcast_to(mine, (H, B)) < 0
    pltpu.make_async_copy(tiles, tiles, tile_sem.at[0]).wait() if tiles.shape[0] == T else pltpu.make_async_copy(
        tiles.at[pl.ds(0, T)], tiles.at[pl.ds(0, T)], tile_sem.at[0]
    ).wait()

    for group, (lo, hi) in enumerate(zip(bounds, bounds[1:])):
        if hi > max(lo, 1):
            landed(lab.at[pl.ds(0, hi - max(lo, 1))], lab_recv.at[group])
        for m in range(max(lo, 1), hi):
            show(col_partner(m))
        if hi > lo:
            for m in range(R - 1, -1, -1):
                k = row_partner(m)
                value = None if lo == 0 else acc0[k]
                for n in range(lo, hi):
                    c = col_partner(n) if n else col
                    part = jnp.dot(hot[c], tile_at(c, k), preferred_element_type=f32)
                    value = part if value is None else value + part
                acc0[k] = value

    for h in range(CHAINS):
        for m in range(R - 1, 0, -1):
            k = row_partner(m)
            send(acc0.at[k, pl.ds(PAD + h * H, H)], rs0.at[h, m - 1], rs0_send.at[0], rs0_recv.at[h], {"row": k})
    for m in range(R - 1, 0, -1):
        k = row_partner(m)
        send(acc0.at[k, pl.ds(PAD - DEG, DEG)], deg.at[m - 1], deg_send.at[0], deg_recv.at[0], {"row": k})

    lead = CHAINS - EARLY

    def slot(t):
        return t // ITERS * 2 + t % ITERS % 2

    def gather_start(t):
        early = t // ITERS >= lead
        own = code.at[t, col]
        for j in range(Z - 1):
            send(own, own, code_send.at[0], code_recv.at[slot(t), chip], {"col": 2 * other_chip(j) + core})
        send(own, own, code_send.at[0], code_recv.at[slot(t), chip], {"col": peer})
        if early:
            for m in range(R - 1, 0, -1):
                send(own, code.at[t, C + row], side_send.at[0], side_recv.at[slot(t - lead * ITERS)], {"row": row_partner(m)})
        own = unit.at[t, col]
        for m in range(C - 1, 0, -1):
            send(own, own, unit_send.at[0], unit_recv.at[slot(t)], {"col": col_partner(m)})
        if early:
            for m in range(R - 1, 0, -1):
                send(own, unit.at[t, C + row], side_send.at[1], unit_recv.at[slot(t)], {"row": row_partner(m)})

    def gather_relay(t, j):
        z = other_chip(j)
        block = code.at[t, 2 * z + core]
        landed(block, code_recv.at[slot(t), z])
        send(block, block, code_send.at[0], code_recv.at[slot(t), chip], {"col": peer})

    def gather_end(t):
        landed(code.at[t, pl.ds(0, Z)], code_recv.at[slot(t), chip])
        if t // ITERS >= lead:
            landed(code.at[t, pl.ds(0, R - 1)], side_recv.at[slot(t - lead * ITERS)])
            landed(unit.at[t, pl.ds(0, C + R - 2)], unit_recv.at[slot(t)])
        else:
            landed(unit.at[t, pl.ds(0, C - 1)], unit_recv.at[slot(t)])

    me = row * C + col

    def stats_start(t, rows):
        for i in range(st.shape[2]):
            st[t, me, i] = rows[i] if i < len(rows) else jnp.zeros((1, K), f32)
        own = st.at[t, me]

        def out(n, carry):
            other = lax.rem(me + n + 1, R * C)
            send(own, own, st_send.at[0], st_recv.at[slot(t)], {"row": lax.div(other, C), "col": lax.rem(other, C)})
            return carry

        if unroll:
            pairs = [(y, z) for y in range(R) for z in range(C)][1:]
            for y, z in sorted(pairs, key=lambda pair: -(pair[0].bit_count() + pair[1] // 2)):
                send(own, own, st_send.at[0], st_recv.at[slot(t)], {"row": row_partner(y), "col": col_partner(z)})
        else:
            lax.fori_loop(0, R * C - 1, out, 0)

    def stats_end(t):
        landed(st.at[t, pl.ds(0, R * C - 1)], st_recv.at[slot(t)])
        return jnp.sum(st[t], axis=0)

    def weigh():
        landed(deg, deg_recv.at[0])
        value = acc0[row, PAD - DEG : PAD]
        for m in range(1, R):
            value = value + deg[m - 1]
        degree[...] = value

    def apply(t, d):
        mixed = acc[t // ITERS, row]
        for m in range(1, R):
            mixed = mixed + unpack(rs[t, m - 1], rg[t, m - 1])
        return jnp.where(free, degree[0:1] * d - mixed, d)

    def chain(h):
        clock = OFFSET * h
        yield clock
        landed(rs0.at[h], rs0_recv.at[h])
        value = acc0[row, PAD + h * H : PAD + (h + 1) * H]
        for m in range(1, R):
            value = value + rs0[h, m - 1]
        rhs = jnp.where(free, value, 0.0)
        encode(h * ITERS, rhs)
        gather_start(h * ITERS)
        answer[h] = jnp.zeros((H, B), f32)
        residual[h] = rhs
        direction[h] = rhs
        norm = None
        for s in range(ITERS):
            t = h * ITERS + s
            last = s + 1 == ITERS
            if Z > 1:
                yield clock + NEAR
                gather_relay(t, Z - 2)
            if Z > 2:
                yield clock + MID
                for j in range(Z - 3, 0, -1):
                    gather_relay(t, j)
                yield clock + FAR
                gather_relay(t, 0)
            yield clock + READY
            if s:
                total = stats_end(t - 1)
                if s == 1:
                    di, ii, norm = spread(total, 3)
                    ri = di
                else:
                    di, ri, ii = spread(total, 3)
                alpha = norm / di
                after = norm - 2.0 * alpha * ri + alpha * alpha * ii
                beta = after / norm
                norm = after
                a, b = wide(alpha), wide(beta)
            gather_end(t)

            def refresh(c, carry, side=False):
                fresh = decode(t, c)
                if s == 0:
                    rep_r[h, c] = fresh
                else:
                    old = rep_r[h, c]
                    r = old - a * fresh
                    p = r + b * (old if s == 1 else rep_p[h, c])
                    if not last:
                        rep_r[h, c] = r
                    if side or not last:
                        rep_p[h, c] = p
                    fresh = p
                if not side:
                    panel[h, c] = fresh.astype(bf16)
                return carry

            loop(C, refresh, 0)

            def ship(m, k, value):
                if m == 0 or (last and h >= lead):
                    acc[h, k] = value
                if m:
                    piece[t, k], grade[t, k] = pack(value)
                    send(piece.at[t, k], rs.at[t, m - 1], rs_send.at[0], rs_recv.at[h], {"row": k})
                    send(grade.at[t, k], rg.at[t, m - 1], rg_send.at[0], rg_recv.at[h], {"row": k})

            held = None
            for m in range(R - 1, -1, -1):
                k = row_partner(m)

                def one(c, value):
                    part = jnp.dot(panel[h, c], tile_at(c, k), preferred_element_type=f32)
                    return part if value is None else value + part

                value = loop(C, one, None if unroll else jnp.zeros((H, B), f32))
                if held is not None:
                    ship(*held)
                held = (m, k, value)
            ship(*held)
            for m in range(1, R if h >= lead else 1):
                refresh(C + row_partner(m), 0, True)
            if s:
                d = direction[h]
                r = residual[h] - a * image[h]
                answer[h] = answer[h] + a * d
                residual[h] = r
                direction[h] = r + b * d
            if last and h >= lead:
                d = direction[h]
                inner = jnp.where(free, degree[0:1] * d, d) * d - d * acc[h, row]
                for m in range(1, R):
                    k = row_partner(m)
                    inner = inner - rep_p[h, C + k] * acc[h, k]
                stats_start(t, sums_row([inner]))
                break
            clock += PERIOD
            yield clock
            if h == 0 and s == 0:
                weigh()
            landed(rs.at[t], rs_recv.at[h])
            landed(rg.at[t], rg_recv.at[h])
            i = apply(t, direction[h])
            image[h] = i
            d, r = direction[h], residual[h]
            if last:
                stats_start(t, sums_row([d * i]))
                break
            encode(t + 1, i)
            gather_start(t + 1)
            stats_start(t, sums_row([d * i, i * i, r * r] if s == 0 else [d * i, r * i, i * i]))
        d = direction[h]
        if h >= lead:
            yield clock + READY + SUMS
            landed(rs.at[t], rs_recv.at[h])
            landed(rg.at[t], rg_recv.at[h])
            i = apply(t, d)
        else:
            yield clock + SUMS
            i = image[h]
        (di,) = spread(stats_end(t), 1)
        a = wide(norm / di)
        out[0:B, h * H : (h + 1) * H] = ((8.0 * K) * (answer[h] + a * d)).T
        out[B : 2 * B, h * H : (h + 1) * H] = (residual[h] - a * i).T

    queue = []
    for h in range(CHAINS):
        one = chain(h)
        queue.append((next(one), h, one))
    while queue:
        queue.sort(key=lambda entry: entry[:2])
        _, h, one = queue.pop(0)
        when = next(one, None)
        if when is not None:
            queue.append((when, h, one))

    drained(lab.at[pl.ds(0, C - 1)], lab_send.at[0])
    drained(code.at[:, pl.ds(0, C - 1)], code_send.at[0])
    drained(unit.at[:, pl.ds(0, C - 1)], unit_send.at[0])
    if EARLY:
        drained(code.at[pl.ds(0, EARLY * ITERS), pl.ds(0, R - 1)], side_send.at[0])
        drained(unit.at[pl.ds(0, EARLY * ITERS), pl.ds(0, R - 1)], side_send.at[1])
    drained(deg, deg_send.at[0])
    drained(rs0, rs0_send.at[0])
    drained(rs, rs_send.at[0])
    drained(rg, rg_send.at[0])
    drained(st.at[:, pl.ds(0, R * C - 1)], st_send.at[0])


def solution(mesh):
    R, C = mesh.shape["row"], mesh.shape["col"]

    def shards(tiles, tile_row, tile_col, label_class):
        T, B = tiles.shape[0], tiles.shape[1]
        K, H, N = CLASSES, CLASSES // CHAINS, CHAINS
        held = T if T == R * C else T + 1
        f32, bf16, i32 = jnp.float32, jnp.bfloat16, jnp.int32
        dma = pltpu.SemaphoreType.DMA
        vmem, hbm = pl.BlockSpec(memory_space=pltpu.VMEM), pl.BlockSpec(memory_space=pltpu.HBM)
        smem = pltpu.SMEM
        node = pltpu.VMEM((N, H, B), f32)
        steps = N * ITERS
        lines = -(-3 // (K // H))
        both = pl.pallas_call(
            functools.partial(kernel, R, C),
            out_shape=jax.ShapeDtypeStruct((2 * B, K), f32),
            in_specs=[
                hbm, hbm, hbm, hbm,
            ],
            out_specs=vmem,
            scratch_shapes=[
                smem((T,), i32), smem((T,), i32), smem((R * C,), i32), pltpu.VMEM((1, B), i32),
                pltpu.VMEM((held, B, B), bf16),
                pltpu.VMEM((C, 1, B), i32),
                pltpu.VMEM((C, PAD + K, B), bf16),
                pltpu.VMEM((R, PAD + K, B), f32),
                pltpu.VMEM((N, R - 1, H, B), f32),
                pltpu.VMEM((R - 1, DEG, B), f32),
                pltpu.VMEM((steps, C + R, H // 2, B), i32),
                pltpu.VMEM((steps, C + R, 1, B), f32),
                pltpu.VMEM((N, C, H, B), bf16),
                pltpu.VMEM((N, C + R, H, B), f32),
                pltpu.VMEM((N, C + R, H, B), f32),
                pltpu.VMEM((N, R, H, B), f32),
                pltpu.VMEM((steps, R, H // 2, B), i32),
                pltpu.VMEM((steps, R, 1, B), f32),
                pltpu.VMEM((steps, R - 1, H // 2, B), i32),
                pltpu.VMEM((steps, R - 1, 1, B), f32),
                pltpu.VMEM((steps, R * C, lines, 1, K), f32),
                pltpu.VMEM((DEG, B), f32),
                node, node, node, node,
                dma((1,)),
                dma((1,)), dma((3,)),
                dma((1,)), dma((2 * N, C // 2)),
                dma((1,)), dma((2 * N,)), dma((2,)), dma((2 * max(EARLY, 1),)),
                dma((1,)), dma((1,)), dma((1,)), dma((N,)),
                dma((1,)), dma((N,)), dma((1,)), dma((N,)),
                dma((1,)), dma((2 * N,)),
                dma((3,)),
            ],
            compiler_params=pltpu.CompilerParams(
                collective_id=0, has_side_effects=True, vmem_limit_bytes=40 * 1024 * 1024
            ),
        )(*(pltpu.with_memory_space_constraint(v, pltpu.HBM) for v in (tile_row, tile_col, label_class.reshape(1, B), tiles)))
        return both[:B], both[B:]

    placed = (P(("row", "col"), None, None),) + (P(("row", "col")),) * 3
    return jax.shard_map(
        shards,
        mesh=mesh,
        in_specs=placed,
        out_specs=(P(("row", "col"), None), P(("row", "col"), None)),
        check_vma=False,
    )
```
